32 devices in a mesh: rep: 1 (over z), data: 32 (over y, x, core).
Axes of the slice: x: 4, y: 4, z: 1, core: 2. Of those that a mesh axis runs over, the one named last changes fastest.
The devices are a block of a 4x4x8 slice.
Arguments:
- x: bfloat16 [2048, 3072], P(('rep', 'data'))
- adapter_id: int32 [2048], P(('rep', 'data'))
- w_gate: bfloat16 [3072, 8192], replicated
- w_up: bfloat16 [3072, 8192], replicated
- w_down: bfloat16 [8192, 3072], replicated
- a_gate: bfloat16 [256, 16, 3072], P('data')
- b_gate: bfloat16 [256, 16, 8192], P('data')
- a_up: bfloat16 [256, 16, 3072], P('data')
- b_up: bfloat16 [256, 16, 8192], P('data')
- a_down: bfloat16 [256, 16, 8192], P('data')
- b_down: bfloat16 [256, 16, 3072], P('data')
Outputs:
- output: bfloat16 [2048, 3072], P(('rep', 'data'))
All inputs are finite; a program needn't handle non-finite values.
Results may differ from the reference program's by a relative error of at most 0.00573171.
Values are sent between devices in bfloat16 or wider.
A program may use at most 768 MiB of HBM per device.

```python
import jax
import jax.numpy as jnp
from jax import lax

D = 3072
FF = 8192
RANK = 16
ADAPTERS = 256
TOK = 64
GROUP = 32
CAP = 6
LORA_ALPHA = 32

SCALE = LORA_ALPHA / RANK
TOKENS = TOK * GROUP
PER_OWNER = ADAPTERS // GROUP


def shuffle_row(row_key, row_owner):
    return row_owner[jax.random.permutation(row_key, TOK)]


def draw_ids(id_key):
    id_keys = jax.random.split(id_key, 5)
    hot_owner = jax.random.randint(id_keys[0], (), 0, GROUP)
    offset = jax.random.randint(id_keys[1], (), 0, GROUP - 1)
    source = jnp.arange(GROUP)[:, None]
    position = jnp.arange(TOK)[None, :]
    spread = (offset + source * (TOK - CAP) + position - CAP) % (GROUP - 1)
    owner_idx = jnp.where(position < CAP, hot_owner, (hot_owner + 1 + spread) % GROUP)
    owner_idx = jax.vmap(shuffle_row)(jax.random.split(id_keys[2], GROUP), owner_idx)
    flat_owner = owner_idx.reshape(TOKENS)
    owner_hot = (flat_owner[:, None] == jnp.arange(GROUP)[None, :]).astype(jnp.int32)
    arrival = jnp.sum(jnp.cumsum(owner_hot, axis=0) * owner_hot, axis=1) - 1
    popular = jnp.minimum(jax.random.randint(id_keys[3], (TOKENS,), 0, PER_OWNER), jax.random.randint(id_keys[4], (TOKENS,), 0, PER_OWNER))
    local_idx = jnp.where(arrival == 0, 0, jnp.where(arrival == 1, PER_OWNER - 1, popular))
    return (flat_owner * PER_OWNER + local_idx).astype(jnp.int32)


def setup_inputs(seed: int = 0, part: int = 0) -> dict:
    key = jax.random.key(seed)
    weight_keys = jax.random.split(key, 9)
    part_keys = jax.random.split(jax.random.fold_in(key, part), 2)
    b_scale = 0.3 / (SCALE * RANK ** 0.5)

    def draw_normal(index, shape, std):
        return (jax.random.normal(weight_keys[index], shape, jnp.float32) * std).astype(jnp.bfloat16)

    return {
        "x": jax.random.normal(part_keys[0], (TOKENS, D), jnp.float32).astype(jnp.bfloat16),
        "adapter_id": draw_ids(part_keys[1]),
        "w_gate": draw_normal(0, (D, FF), D ** -0.5),
        "w_up": draw_normal(1, (D, FF), D ** -0.5),
        "w_down": draw_normal(2, (FF, D), FF ** -0.5),
        "a_gate": draw_normal(3, (ADAPTERS, RANK, D), D ** -0.5),
        "b_gate": draw_normal(4, (ADAPTERS, RANK, FF), b_scale),
        "a_up": draw_normal(5, (ADAPTERS, RANK, D), D ** -0.5),
        "b_up": draw_normal(6, (ADAPTERS, RANK, FF), b_scale),
        "a_down": draw_normal(7, (ADAPTERS, RANK, FF), FF ** -0.5),
        "b_down": draw_normal(8, (ADAPTERS, RANK, D), b_scale),
    }


def lora_delta(tok_rows, tok_ids, a_mat, b_mat):
    a_rows = a_mat[tok_ids].astype(jnp.float32)
    b_rows = b_mat[tok_ids].astype(jnp.float32)
    low_rank = jnp.einsum("td,trd->tr", tok_rows.astype(jnp.float32), a_rows).astype(jnp.bfloat16)
    full_rows = jnp.einsum("tr,trf->tf", low_rank.astype(jnp.float32), b_rows)
    return (SCALE * full_rows).astype(jnp.bfloat16)


def reference(x, adapter_id, w_gate, w_up, w_down, a_gate, b_gate, a_up, b_up, a_down, b_down):
    def one_block(block_in):
        tok_rows, tok_ids = block_in
        gate_pre = jnp.dot(tok_rows, w_gate, preferred_element_type=jnp.float32) + lora_delta(tok_rows, tok_ids, a_gate, b_gate).astype(jnp.float32)
        up_pre = jnp.dot(tok_rows, w_up, preferred_element_type=jnp.float32) + lora_delta(tok_rows, tok_ids, a_up, b_up).astype(jnp.float32)
        hidden = (jax.nn.silu(gate_pre) * up_pre).astype(jnp.bfloat16)
        down_out = jnp.dot(hidden, w_down, preferred_element_type=jnp.float32) + lora_delta(hidden, tok_ids, a_down, b_down).astype(jnp.float32)
        return (tok_rows.astype(jnp.float32) + down_out).astype(jnp.bfloat16)

    blocks = (x.reshape(GROUP, TOK, D), adapter_id.reshape(GROUP, TOK))
    return lax.map(one_block, blocks).reshape(TOKENS, D)
```

```python
import jax
import jax.numpy as jnp
from jax import lax
from jax.sharding import PartitionSpec as P

LORA_ALPHA = 32


def solution(mesh):
    groups = mesh.shape["data"]
    row_spec = P(("rep", "data"), None)
    id_spec = P(("rep", "data"))
    owned_spec = P("data", None, None)

    def device_step(x, adapter_id, w_gate, w_up, w_down, a_gate, b_gate, a_up, b_up, a_down, b_down):
        tok, dim = x.shape
        per_owner, rank, _ = a_gate.shape
        scale = LORA_ALPHA / rank
        cap = (3 * tok + groups - 1) // groups
        stack = per_owner * rank
        owner = adapter_id // per_owner
        local = adapter_id % per_owner
        owner_hot = (owner[:, None] == jnp.arange(groups)[None, :]).astype(jnp.int32)
        arrival = jnp.sum(jnp.cumsum(owner_hot, axis=0) * owner_hot, axis=1) - 1
        slot = owner * cap + arrival
        dispatch = (slot[:, None] == jnp.arange(groups * cap)[None, :]).astype(jnp.bfloat16)
        mine = (local[:, None] == (jnp.arange(stack) // rank)[None, :]).astype(jnp.bfloat16)
        rows = jnp.concatenate([x, mine], axis=1)
        send = jnp.einsum("tm,td->md", dispatch, rows, preferred_element_type=jnp.float32).astype(jnp.bfloat16)
        recv = lax.all_to_all(send, "data", 0, 0, tiled=True)
        xr, keep = recv[:, :dim], recv[:, dim:] > 0

        def delta(v, a, b):
            low = jnp.einsum("md,rd->mr", v, a.reshape(stack, -1), preferred_element_type=jnp.float32)
            low = jnp.where(keep, low.astype(jnp.bfloat16), jnp.bfloat16(0))
            full = jnp.dot(low, b.reshape(stack, -1), preferred_element_type=jnp.float32)
            return (scale * full).astype(jnp.bfloat16).astype(jnp.float32)

        gate = jnp.dot(xr, w_gate, preferred_element_type=jnp.float32) + delta(xr, a_gate, b_gate)
        up = jnp.dot(xr, w_up, preferred_element_type=jnp.float32) + delta(xr, a_up, b_up)
        hidden = (jax.nn.silu(gate) * up).astype(jnp.bfloat16)
        down = jnp.dot(hidden, w_down, preferred_element_type=jnp.float32) + delta(hidden, a_down, b_down)
        out = (xr.astype(jnp.float32) + down).astype(jnp.bfloat16)
        back = lax.all_to_all(out, "data", 0, 0, tiled=True)
        return jnp.einsum("tm,md->td", dispatch, back, preferred_element_type=jnp.float32).astype(jnp.bfloat16)

    return jax.shard_map(device_step, mesh=mesh, in_specs=(row_spec, id_spec, P(), P(), P(), owned_spec, owned_spec, owned_spec, owned_spec, owned_spec, owned_spec), out_specs=row_spec, check_vma=False)
```

```python
import functools
import math

import jax
import jax.numpy as jnp
from jax import lax
from jax.experimental import pallas as pl
from jax.experimental.pallas import tpu as pltpu
from jax.sharding import PartitionSpec as P

LORA_ALPHA = 32
BF, F32 = jnp.bfloat16, jnp.float32
CORES = 2
UNIT_K, UNIT_N = 1024, 512
UNITS = 36
MAIN = 384


def one_hot(rows, cols, hit):
    r = lax.broadcasted_iota(jnp.int32, (rows, cols), 0)
    c = lax.broadcasted_iota(jnp.int32, (rows, cols), 1)
    return hit(r, c).astype(F32).astype(BF)


def dot(a, b):
    return jnp.dot(a, b, preferred_element_type=F32)


def dot_t(a, b):
    return lax.dot_general(a, b, (((1,), (1,)), ((), ())), preferred_element_type=F32)


def layer(groups, cap, scale, rank, ids_ref, x_hbm, wg_hbm, wu_hbm, wd_hbm, ag_hbm, bg_hbm, au_hbm, bu_hbm, ad_hbm, bd_hbm, out_hbm,
          ring, x_v, xc, h_v, agu, bgu, adv, bdv, send1, recv1, send2, recv2, o_v, keep_v, low_v, gmat,
          ring_sem, in_sem, s1_sem, r1_sem, s2_sem, r2_sem):
    tok, dim = x_v.shape
    ff = h_v.shape[1]
    stack = bdv.shape[0]
    slots = groups * cap
    slab = send1.shape[1]
    packed = groups * slab
    side = math.isqrt(groups // CORES)
    n_in = ff // UNIT_N
    k_in = dim // UNIT_K
    n_out = dim // UNIT_N
    k_out = ff // UNIT_K
    in_units = n_in * 2 * k_in
    me = lax.axis_index("data")
    my_c, my_x, my_y = lax.rem(me, CORES), lax.rem(me // CORES, side), me // (CORES * side)

    def target(r, back=False):
        dy, dx, dc = r // (CORES * side), (r // CORES) % side, r % CORES
        if back:
            dy, dx = (side - dy) % side, (side - dx) % side
        return {"data": (lax.rem(my_y + dy, side) * side + lax.rem(my_x + dx, side)) * CORES + lax.rem(my_c + dc, CORES)}

    def in_copy(src, dst, i):
        return pltpu.make_async_copy(src, dst, in_sem.at[i])

    def in_unit(j, which, k, slot):
        src = (wg_hbm, wu_hbm)[which]
        col = pl.multiple_of(j * UNIT_N, UNIT_N)
        return pltpu.make_async_copy(src.at[pl.ds(k * UNIT_K, UNIT_K), pl.ds(col, UNIT_N)], ring.at[slot], ring_sem.at[slot])

    def out_unit(n, k, slot):
        col = pl.multiple_of(n * UNIT_N, UNIT_N)
        row = pl.multiple_of(k * UNIT_K, UNIT_K)
        return pltpu.make_async_copy(wd_hbm.at[pl.ds(row, UNIT_K), pl.ds(col, UNIT_N)], ring.at[slot], ring_sem.at[slot])

    half = agu.shape[0] // 2
    x_copy = in_copy(x_hbm, x_v, 0)
    x_copy.start()
    early = [in_copy(ag_hbm, agu.at[pl.ds(0, half)], 1), in_copy(au_hbm, agu.at[pl.ds(half, half)], 2),
             in_copy(bg_hbm, bgu.at[0], 3), in_copy(bu_hbm, bgu.at[1], 4)]
    late = [in_copy(ad_hbm, adv, 5), in_copy(bd_hbm, bdv, 6)]
    for c in early:
        c.start()
    per = 2 * k_in
    for u in range(UNITS):
        in_unit(u // per, (u % per) // k_in, u % k_in, u).start()
    for c in late:
        c.start()

    barrier = pltpu.get_barrier_semaphore()
    for r in range(1, groups):
        pl.semaphore_signal(barrier, inc=1, device_id=target(r), device_id_type=pl.DeviceIdType.MESH)

    ids = ids_ref[...].astype(F32)
    eye = lax.broadcasted_iota(jnp.int32, (tok, tok), 0) == lax.broadcasted_iota(jnp.int32, (tok, tok), 1)
    ids_c = jnp.sum(jnp.where(eye, jnp.broadcast_to(ids, (tok, tok)), 0.0), axis=1, keepdims=True)
    per_owner = stack // rank

    def fdiv(v, n):
        return jnp.floor((v + 0.5) * (1.0 / n))

    def place(v):
        owner = fdiv(v, per_owner)
        local = v - owner * per_owner
        oy = fdiv(owner, CORES * side)
        ox = fdiv(owner, CORES) - oy * side
        oc = owner - fdiv(owner, CORES) * CORES

        def mod(a, b, n):
            d = a - b.astype(F32)
            return jnp.where(d < 0, d + n, d)
        rel = (mod(oy, my_y, side) * side + mod(ox, my_x, side)) * CORES + mod(oc, my_c, CORES)
        return owner, local, rel

    own_r, _, rel_r = place(ids)
    own_c, loc_c, rel_c = place(ids_c)
    t0 = lax.broadcasted_iota(jnp.int32, (tok, tok), 0)
    t1 = lax.broadcasted_iota(jnp.int32, (tok, tok), 1)
    same = own_c == own_r
    arr_r = jnp.sum(jnp.where(same & (t0 < t1), 1.0, 0.0), axis=0, keepdims=True)
    arr_c = jnp.sum(jnp.where(same & (t1 < t0), 1.0, 0.0), axis=1, keepdims=True)
    third = cap // 2

    def rows_of(rel, arr):
        main = (rel * slab + arr).astype(jnp.int32)
        tail_row = fdiv(arr, third)
        tail = (rel * slab + cap + tail_row).astype(jnp.int32)
        part = (arr - tail_row * third).astype(jnp.int32)
        return main, tail, part

    main_r, tail_r, part_r = rows_of(rel_r, arr_r)
    main_c, tail_c, part_c = rows_of(rel_c, arr_c)
    s_main = one_hot(packed, tok, lambda r, c: r == main_r)
    s_tail = [one_hot(packed, tok, lambda r, c: (r == tail_r) & (part_r == k)) for k in range(third)]
    gmat[0] = one_hot(tok, packed, lambda r, c: c == main_c)
    for k in range(third):
        gmat[1 + k] = one_hot(tok, packed, lambda r, c: (c == tail_c) & (part_c == k))
    mine = one_hot(tok, stack, lambda r, c: loc_c == fdiv(c.astype(F32), rank))

    x_copy.wait()
    mask0 = n_out * MAIN
    for n in range(n_out):
        xa = x_v[:, n * UNIT_N:n * UNIT_N + MAIN]
        xb = x_v[:, n * UNIT_N + MAIN:(n + 1) * UNIT_N]
        both = dot(s_main, xa) + jnp.concatenate([dot(s, xb) for s in s_tail], axis=1)
        send1[:, :, n * MAIN:(n + 1) * MAIN] = both.reshape(groups, slab, MAIN).astype(BF)
    send1[:, :, mask0:] = dot(s_main, mine).reshape(groups, slab, stack).astype(BF)

    pl.semaphore_wait(barrier, groups - 1)

    def copy1(r):
        return pltpu.make_async_remote_copy(send1.at[r], recv1.at[r], s1_sem.at[r], r1_sem.at[r], device_id=target(r), device_id_type=pl.DeviceIdType.MESH)

    for r in range(1, groups):
        copy1(r).start()
    recv1[0] = send1[0]

    def slot_of(s):
        g = fdiv(s.astype(F32), cap).astype(jnp.int32)
        return g, s - g * cap

    def unpack_main(r, c):
        g, j = slot_of(r)
        return c == g * slab + j

    def unpack_tail(k):
        def hit(r, c):
            g, j = slot_of(r)
            q = fdiv(j.astype(F32), third).astype(jnp.int32)
            return (c == g * slab + cap + q) & (j - q * third == k)
        return hit

    def pack_main(r, c):
        return unpack_main(c, r)

    def pack_tail(k):
        def hit(r, c):
            return unpack_tail(k)(c, r)
        return hit

    p_main = one_hot(slots, packed, unpack_main)
    p_tail = [one_hot(slots, packed, unpack_tail(k)) for k in range(third)]

    def lanes(ref, at, width):
        return ref[:, :, at:at + width].astype(F32).reshape(packed, width).astype(BF)

    for r in range(1, groups):
        copy1(r).wait()
    for n in range(n_out):
        part = lanes(recv1, n * MAIN, MAIN)
        xc[:, n * UNIT_N:n * UNIT_N + MAIN] = dot(p_main, part).astype(BF)
        w = MAIN // third
        tail = sum(dot(p_tail[k], part[:, k * w:(k + 1) * w]) for k in range(third))
        xc[:, n * UNIT_N + MAIN:(n + 1) * UNIT_N] = tail.astype(BF)
    keep_v[...] = dot(p_main, lanes(recv1, mask0, stack))

    for c in early:
        c.wait()
    keep = keep_v[...] > 0.5
    low = dot_t(xc[...], agu[...])
    for i in range(2):
        low_v[i] = jnp.where(keep, low[:, i * stack:(i + 1) * stack].astype(BF).astype(F32), 0.0).astype(BF)

    blocks = 2
    step_units = blocks * per

    def in_step(i, carry):
        base = i * step_units
        for k in range(step_units):
            slot = lax.rem(base + k, UNITS)
            in_unit(0, 0, 0, slot).wait()
        for b in range(blocks):
            j = i * blocks + b
            for s in range(UNIT_N // 256):
                res = []
                for which in range(2):
                    acc = None
                    for k in range(k_in):
                        slot = lax.rem(base + b * per + which * k_in + k, UNITS)
                        d = dot(xc[:, k * UNIT_K:(k + 1) * UNIT_K], ring[slot, :, s * 256:(s + 1) * 256])
                        acc = d if acc is None else acc + d
                    col = pl.multiple_of(j * UNIT_N + s * 256, 256)
                    delta = (scale * dot(low_v[which], bgu[which, :, pl.ds(col, 256)])).astype(BF).astype(F32)
                    res.append(acc + delta)
                g, u = res
                h_v[:, pl.ds(col, 256)] = (g * (1.0 / (1.0 + jnp.exp(-g))) * u).astype(BF)
        nxt = base + UNITS

        @pl.when(nxt < in_units)
        def _():
            for k in range(step_units):
                in_unit(lax.div(nxt, per) + k // per, (k % per) // k_in, k % k_in, lax.rem(base + k, UNITS)).start()

        @pl.when(nxt >= in_units)
        def _():
            for k in range(step_units):
                v = nxt - in_units + k
                out_unit(lax.div(v, k_out), lax.rem(v, k_out), lax.rem(base + k, UNITS)).start()
        return carry

    lax.fori_loop(0, n_in // blocks, in_step, 0)

    for c in late:
        c.wait()
    low = dot_t(h_v[...], adv[...])
    low_v[0] = jnp.where(keep_v[...] > 0.5, low.astype(BF).astype(F32), 0.0).astype(BF)
    e_main = one_hot(packed, slots, pack_main)
    e_tail = [one_hot(packed, slots, pack_tail(k)) for k in range(third)]

    def copy2(n, r):
        return pltpu.make_async_remote_copy(send2.at[n, r], recv2.at[n, r], s2_sem.at[n, r], r2_sem.at[n, r], device_id=target(r, True), device_id_type=pl.DeviceIdType.MESH)

    total = in_units + n_out * k_out
    for n in range(n_out):
        base = in_units + n * k_out
        for k in range(k_out):
            out_unit(n, k, (base + k) % UNITS).wait()
        cols = slice(n * UNIT_N, (n + 1) * UNIT_N)
        acc = None
        for k in range(k_out):
            d = dot(h_v[:, k * UNIT_K:(k + 1) * UNIT_K], ring[(base + k) % UNITS])
            acc = d if acc is None else acc + d
        delta = (scale * dot(low_v[0], bdv[:, cols])).astype(BF).astype(F32)
        done = (xc[:, cols].astype(F32) + (acc + delta)).astype(BF)
        both = dot(e_main, done[:, :MAIN]) + jnp.concatenate([dot(e, done[:, MAIN:]) for e in e_tail], axis=1)
        send2[n] = both.reshape(groups, slab, MAIN).astype(BF)
        for r in range(1, groups):
            copy2(n, r).start()
        recv2[n, 0] = send2[n, 0]
        for k in range(k_out):
            u = base + k + UNITS
            if u < total:
                out_unit((u - in_units) // k_out, (u - in_units) % k_out, u % UNITS).start()

    for n in range(n_out):
        for r in range(1, groups):
            copy2(n, r).wait()
        part = recv2[n].astype(F32).reshape(packed, MAIN).astype(BF)
        w = MAIN // third
        o_v[:, n * UNIT_N:n * UNIT_N + MAIN] = dot(gmat[0], part).astype(BF)
        tail = sum(dot(gmat[1 + k], part[:, k * w:(k + 1) * w]) for k in range(third))
        o_v[:, n * UNIT_N + MAIN:(n + 1) * UNIT_N] = tail.astype(BF)
    last = in_copy(o_v, out_hbm, 7)
    last.start()
    last.wait()


def solution(mesh):
    groups = mesh.shape["data"]
    row_spec = P(("rep", "data"), None)
    id_spec = P(("rep", "data"))
    owned_spec = P("data", None, None)

    def device_step(x, adapter_id, w_gate, w_up, w_down, a_gate, b_gate, a_up, b_up, a_down, b_down):
        tok, dim = x.shape
        ff = w_gate.shape[1]
        per_owner, rank, _ = a_gate.shape
        stack = per_owner * rank
        cap = (3 * tok + groups - 1) // groups
        slots = groups * cap
        slab = 8
        n_out = dim // UNIT_N
        width = n_out * MAIN + stack
        flat = [m.reshape(stack, m.shape[2]) for m in (a_gate, b_gate, a_up, b_up, a_down, b_down)]
        anyspec = pl.BlockSpec(memory_space=pl.ANY)
        dma = pltpu.SemaphoreType.DMA
        return pl.pallas_call(
            functools.partial(layer, groups, cap, LORA_ALPHA / rank, rank),
            out_shape=jax.ShapeDtypeStruct((tok, dim), BF),
            in_specs=[pl.BlockSpec(memory_space=pltpu.VMEM)] + [anyspec] * 10,
            out_specs=anyspec,
            scratch_shapes=[
                pltpu.VMEM((UNITS, UNIT_K, UNIT_N), BF),
                pltpu.VMEM((tok, dim), BF),
                pltpu.VMEM((slots, dim), BF),
                pltpu.VMEM((slots, ff), BF),
                pltpu.VMEM((2 * stack, dim), BF),
                pltpu.VMEM((2, stack, ff), BF),
                pltpu.VMEM((stack, ff), BF),
                pltpu.VMEM((stack, dim), BF),
                pltpu.VMEM((groups, slab, width), BF),
                pltpu.VMEM((groups, slab, width), BF),
                pltpu.VMEM((n_out, groups, slab, MAIN), BF),
                pltpu.VMEM((n_out, groups, slab, MAIN), BF),
                pltpu.VMEM((tok, dim), BF),
                pltpu.VMEM((slots, stack), F32),
                pltpu.VMEM((2, slots, stack), BF),
                pltpu.VMEM((1 + cap // 2, tok, groups * slab), BF),
                dma((UNITS,)), dma((8,)), dma((groups,)), dma((groups,)), dma((n_out, groups)), dma((n_out, groups)),
            ],
            compiler_params=pltpu.CompilerParams(collective_id=0, has_side_effects=True, vmem_limit_bytes=67043328),
            name="lora_swiglu",
        )(adapter_id.reshape(1, tok), x, w_gate, w_up, w_down, *flat)

    return jax.shard_map(device_step, mesh=mesh, in_specs=(row_spec, id_spec, P(), P(), P(), owned_spec, owned_spec, owned_spec, owned_spec, owned_spec, owned_spec), out_specs=row_spec, check_vma=False)
```

```python
import functools
import math

import jax
import jax.numpy as jnp
from jax import lax
from jax.experimental import pallas as pl
from jax.experimental.pallas import tpu as pltpu
from jax.sharding import PartitionSpec as P

LORA_ALPHA = 32
BF, F32 = jnp.bfloat16, jnp.float32
CORES = 2
UNIT_K, UNIT_N = 1024, 512
UNITS = 32
MAIN = 384


def one_hot(rows, cols, hit):
    r = lax.broadcasted_iota(jnp.int32, (rows, cols), 0)
    c = lax.broadcasted_iota(jnp.int32, (rows, cols), 1)
    return hit(r, c).astype(F32).astype(BF)


def dot(a, b):
    return jnp.dot(a, b, preferred_element_type=F32)


def dot_t(a, b):
    return lax.dot_general(a, b, (((1,), (1,)), ((), ())), preferred_element_type=F32)


def layer(groups, cap, scale, rank, ids_ref, x_hbm, wg_hbm, wu_hbm, wd_hbm, ag_hbm, bg_hbm, au_hbm, bu_hbm, ad_hbm, bd_hbm, out_hbm,
          ring, acc_v, x_v, xc, h_v, bgu, adv, bdv, send0, recv0, send1, recv1, recv2, keep_v, low_v, gmat,
          ring_sem, in_sem, s1_sem, r1_sem, s2_sem, r2_sem):
    tok, dim = x_v.shape
    ff = h_v.shape[1]
    stack = bdv.shape[0]
    slots = groups * cap
    slab = recv0.shape[1]
    packed = groups * slab
    side = math.isqrt(groups // CORES)
    third = cap // 2
    n_in = ff // UNIT_N
    k_in = dim // UNIT_K
    n_out = dim // UNIT_N
    k_out = ff // UNIT_K
    chunks = UNIT_K // UNIT_N
    me = lax.axis_index("data")
    my_c, my_x, my_y = lax.rem(me, CORES), lax.rem(me // CORES, side), me // (CORES * side)

    def target(r, back=False):
        dy, dx, dc = r // (CORES * side), (r // CORES) % side, r % CORES
        if back:
            dy, dx = (side - dy) % side, (side - dx) % side
        return {"data": (lax.rem(my_y + dy, side) * side + lax.rem(my_x + dx, side)) * CORES + lax.rem(my_c + dc, CORES)}

    def in_copy(src, dst, i):
        return pltpu.make_async_copy(src, dst, in_sem.at[i])

    def in_unit(kk, j, which, slot):
        src = (wg_hbm, wu_hbm)[which]
        col = pl.multiple_of(j * UNIT_N, UNIT_N)
        return pltpu.make_async_copy(src.at[pl.ds(kk * UNIT_K, UNIT_K), pl.ds(col, UNIT_N)], ring.at[slot], ring_sem.at[slot])

    def out_unit(n, k, slot):
        col = pl.multiple_of(n * UNIT_N, UNIT_N)
        return pltpu.make_async_copy(wd_hbm.at[pl.ds(k * UNIT_K, UNIT_K), pl.ds(col, UNIT_N)], ring.at[slot], ring_sem.at[slot])

    x_copy = in_copy(x_hbm, x_v, 0)
    x_copy.start()
    early = [in_copy(ag_hbm, h_v.at[pl.ds(0, stack), pl.ds(0, dim)], 1), in_copy(au_hbm, h_v.at[pl.ds(0, stack), pl.ds(dim, dim)], 2),
             in_copy(bg_hbm, bgu.at[0], 3), in_copy(bu_hbm, bgu.at[1], 4)]
    late = [in_copy(ad_hbm, adv, 5), in_copy(bd_hbm, bdv, 6)]
    first = 4
    for u in range(first):
        in_unit(0, u // 2, u % 2, u).start()

    with jax.named_scope("signal"):
        barrier = pltpu.get_barrier_semaphore()
        for r in range(1, groups):
            pl.semaphore_signal(barrier, inc=1, device_id=target(r), device_id_type=pl.DeviceIdType.MESH)

    with jax.named_scope("place"):
        ids = ids_ref[...].astype(F32)
        eye = lax.broadcasted_iota(jnp.int32, (tok, tok), 0) == lax.broadcasted_iota(jnp.int32, (tok, tok), 1)
        ids_c = jnp.sum(jnp.where(eye, jnp.broadcast_to(ids, (tok, tok)), 0.0), axis=1, keepdims=True)
        per_owner = stack // rank

        def fdiv(v, n):
            return jnp.floor((v + 0.5) * (1.0 / n))

        def place(v):
            owner = fdiv(v, per_owner)
            local = v - owner * per_owner
            oy = fdiv(owner, CORES * side)
            ox = fdiv(owner, CORES) - oy * side
            oc = owner - fdiv(owner, CORES) * CORES

            def mod(a, b, n):
                d = a - b.astype(F32)
                return jnp.where(d < 0, d + n, d)
            rel = (mod(oy, my_y, side) * side + mod(ox, my_x, side)) * CORES + mod(oc, my_c, CORES)
            return owner, local, rel

        own_r, _, rel_r = place(ids)
        own_c, loc_c, rel_c = place(ids_c)
        t0 = lax.broadcasted_iota(jnp.int32, (tok, tok), 0)
        t1 = lax.broadcasted_iota(jnp.int32, (tok, tok), 1)
        same = own_c == own_r
        arr_r = jnp.sum(jnp.where(same & (t0 < t1), 1.0, 0.0), axis=0, keepdims=True)
        arr_c = jnp.sum(jnp.where(same & (t1 < t0), 1.0, 0.0), axis=1, keepdims=True)

        def rows_of(rel, arr):
            main = (rel * slab + arr).astype(jnp.int32)
            tail_row = fdiv(arr, third)
            tail = (rel * slab + cap + tail_row).astype(jnp.int32)
            part = (arr - tail_row * third).astype(jnp.int32)
            return main, tail, part

        main_r, tail_r, part_r = rows_of(rel_r, arr_r)
        main_c, tail_c, part_c = rows_of(rel_c, arr_c)
        s_main = one_hot(packed, tok, lambda r, c: r == main_r)
        s_tail = [one_hot(packed, tok, lambda r, c: (r == tail_r) & (part_r == k)) for k in range(third)]
        gmat[0] = one_hot(tok, packed, lambda r, c: c == main_c)
        for k in range(third):
            gmat[1 + k] = one_hot(tok, packed, lambda r, c: (c == tail_c) & (part_c == k))
        mine = one_hot(tok, stack, lambda r, c: loc_c == fdiv(c.astype(F32), rank))

    with jax.named_scope("x_wait"):
        x_copy.wait()
    with jax.named_scope("weights"):
        for u in range(first, UNITS):
            in_unit(0, u // 2, u % 2, u).start()
        for c in early:
            c.start()
        for c in late:
            c.start()

    def sends(kk):
        return send0 if kk == 0 else send1.at[kk - 1]

    def recvs(kk):
        return recv0 if kk == 0 else recv1.at[kk - 1]

    def copy1(kk, r):
        return pltpu.make_async_remote_copy(sends(kk).at[r], recvs(kk).at[r], s1_sem.at[kk, r], r1_sem.at[kk, r], device_id=target(r), device_id_type=pl.DeviceIdType.MESH)

    mask0 = chunks * MAIN
    for kk in range(k_in):
        with jax.named_scope(f"pack{kk}"):
            for b in range(chunks):
                at = kk * UNIT_K + b * UNIT_N
                xa = x_v[:, at:at + MAIN]
                xb = x_v[:, at + MAIN:at + UNIT_N]
                both = dot(s_main, xa) + jnp.concatenate([dot(s, xb) for s in s_tail], axis=1)
                sends(kk)[:, :, b * MAIN:(b + 1) * MAIN] = both.reshape(groups, slab, MAIN).astype(BF)
            if kk == 0:
                send0[:, :, mask0:] = dot(s_main, mine).reshape(groups, slab, stack).astype(BF)
        if kk == 0:
            with jax.named_scope("bar_wait"):
                pl.semaphore_wait(barrier, groups - 1)
        with jax.named_scope(f"send{kk}"):
            for r in range(1, groups):
                copy1(kk, r).start()
            recvs(kk)[0] = sends(kk)[0]

    def slot_of(s):
        g = fdiv(s.astype(F32), cap).astype(jnp.int32)
        return g, s - g * cap

    def unpack_main(r, c):
        g, j = slot_of(r)
        return c == g * slab + j

    def unpack_tail(k):
        def hit(r, c):
            g, j = slot_of(r)
            q = fdiv(j.astype(F32), third).astype(jnp.int32)
            return (c == g * slab + cap + q) & (j - q * third == k)
        return hit

    def pack_main(r, c):
        return unpack_main(c, r)

    def pack_tail(k):
        def hit(r, c):
            return unpack_tail(k)(c, r)
        return hit

    with jax.named_scope("maps"):
        p_main = one_hot(slots, packed, unpack_main)
        p_tail = [one_hot(slots, packed, unpack_tail(k)) for k in range(third)]
    w = MAIN // third

    def lanes(ref, at, width):
        return ref[:, :, at:at + width].astype(F32).reshape(packed, width).astype(BF)

    def arrive(kk):
        with jax.named_scope(f"recv{kk}"):
            for r in range(1, groups):
                copy1(kk, r).wait()
        with jax.named_scope(f"unpack{kk}"):
            for b in range(chunks):
                at = kk * UNIT_K + b * UNIT_N
                part = lanes(recvs(kk), b * MAIN, MAIN)
                xc[:, at:at + MAIN] = dot(p_main, part).astype(BF)
                tail = sum(dot(p_tail[k], part[:, k * w:(k + 1) * w]) for k in range(third))
                xc[:, at + MAIN:at + UNIT_N] = tail.astype(BF)
            if kk == 0:
                keep_v[...] = dot(p_main, lanes(recv0, mask0, stack))

    def low_rank(v, a, i):
        low = dot_t(v, a)
        low_v[i] = jnp.where(keep_v[...] > 0.5, low.astype(BF).astype(F32), 0.0).astype(BF)

    blocks = 4
    per_step = 2 * blocks
    steps = n_in // blocks
    for kk in range(k_in):
        arrive(kk)
        if kk == k_in - 1:
            with jax.named_scope("low"):
                for c in early:
                    c.wait()
                for i in range(2):
                    low_rank(xc[...], h_v[0:stack, i * dim:(i + 1) * dim], i)

        def step(i, carry):
            base = i * per_step
            for k in range(per_step):
                in_unit(0, 0, 0, base + k).wait()
            with jax.named_scope(f"dot{kk}"):
                for b in range(blocks):
                    for s in range(UNIT_N // 256):
                        col = pl.ds(pl.multiple_of((i * blocks + b) * UNIT_N + s * 256, 256), 256)
                        res = []
                        for which in range(2):
                            d = dot(xc[:, kk * UNIT_K:(kk + 1) * UNIT_K], ring[base + b * 2 + which, :, s * 256:(s + 1) * 256])
                            if kk > 0:
                                d = acc_v[which, :, col] + d
                            if kk < k_in - 1:
                                acc_v[which, :, col] = d
                            else:
                                res.append(d + (scale * dot(low_v[which], bgu[which, :, col])).astype(BF).astype(F32))
                        if res:
                            g, u = res
                            h_v[:, col] = (g * (1.0 / (1.0 + jnp.exp(-g))) * u).astype(BF)
            for k in range(per_step):
                if kk < k_in - 1:
                    in_unit(kk + 1, i * blocks + k // 2, k % 2, base + k).start()
                else:
                    out_unit(i, k, base + k).start()
            return carry

        lax.fori_loop(0, steps, step, 0)

    with jax.named_scope("low2"):
        for c in late:
            c.wait()
        low_rank(h_v[...], adv[...], 0)
        e_main = one_hot(packed, slots, pack_main)
        e_tail = [one_hot(packed, slots, pack_tail(k)) for k in range(third)]

    def sent2(n):
        return send1.at[n % 2, :, :, pl.ds(n // 2 % chunks * MAIN, MAIN)]

    def copy2(n, r):
        return pltpu.make_async_remote_copy(sent2(n).at[r], recv2.at[n, r], s2_sem.at[n, r], r2_sem.at[n, r], device_id=target(r, True), device_id_type=pl.DeviceIdType.MESH)

    def ship(n):
        with jax.named_scope(f"ship{n}"):
            for r in range(1, groups):
                copy2(n, r).start()

    def home(n):
        with jax.named_scope(f"homewait{n}"):
            for r in range(1, groups):
                copy2(n, r).wait()
        with jax.named_scope(f"home{n}"):
            part = recv2[n].astype(F32).reshape(packed, MAIN).astype(BF)
            x_v[:, n * UNIT_N:n * UNIT_N + MAIN] = dot(gmat[0], part).astype(BF)
            tail = sum(dot(gmat[1 + k], part[:, k * w:(k + 1) * w]) for k in range(third))
            x_v[:, n * UNIT_N + MAIN:(n + 1) * UNIT_N] = tail.astype(BF)

    for n in range(n_out):
        base = n * k_out
        for k in range(k_out):
            out_unit(n, k, (base + k) % UNITS).wait()
        if n > 0:
            ship(n - 1)
        with jax.named_scope(f"out{n}"):
            done = []
            for s in range(UNIT_N // 256):
                cols = slice(n * UNIT_N + s * 256, n * UNIT_N + (s + 1) * 256)
                acc = None
                for k in range(k_out):
                    d = dot(h_v[:, k * UNIT_K:(k + 1) * UNIT_K], ring[(base + k) % UNITS, :, s * 256:(s + 1) * 256])
                    acc = d if acc is None else acc + d
                delta = (scale * dot(low_v[0], bdv[:, cols])).astype(BF).astype(F32)
                done.append((xc[:, cols].astype(F32) + (acc + delta)).astype(BF))
            done = jnp.concatenate(done, axis=1)
            both = dot(e_main, done[:, :MAIN]) + jnp.concatenate([dot(e, done[:, MAIN:]) for e in e_tail], axis=1)
            sent2(n)[...] = both.reshape(groups, slab, MAIN).astype(BF)
            recv2[n, 0] = sent2(n)[0]
        ahead = n + UNITS // k_out
        for k in range(k_out):
            if ahead < n_out:
                out_unit(ahead, k, (base + k) % UNITS).start()
        if n > 2:
            home(n - 3)
    ship(n_out - 1)
    for n in range(n_out - 3, n_out):
        home(n)
    last = in_copy(x_v, out_hbm, 7)
    last.start()
    last.wait()


def solution(mesh):
    groups = mesh.shape["data"]
    row_spec = P(("rep", "data"), None)
    id_spec = P(("rep", "data"))
    owned_spec = P("data", None, None)

    def device_step(x, adapter_id, w_gate, w_up, w_down, a_gate, b_gate, a_up, b_up, a_down, b_down):
        tok, dim = x.shape
        ff = w_gate.shape[1]
        per_owner, rank, _ = a_gate.shape
        stack = per_owner * rank
        cap = (3 * tok + groups - 1) // groups
        slots = groups * cap
        slab = 8
        n_out = dim // UNIT_N
        k_in = dim // UNIT_K
        width = UNIT_K // UNIT_N * MAIN
        flat = [m.reshape(stack, m.shape[2]) for m in (a_gate, b_gate, a_up, b_up, a_down, b_down)]
        anyspec = pl.BlockSpec(memory_space=pl.ANY)
        dma = pltpu.SemaphoreType.DMA
        return pl.pallas_call(
            functools.partial(layer, groups, cap, LORA_ALPHA / rank, rank),
            out_shape=jax.ShapeDtypeStruct((tok, dim), BF),
            in_specs=[pl.BlockSpec(memory_space=pltpu.VMEM)] + [anyspec] * 10,
            out_specs=anyspec,
            scratch_shapes=[
                pltpu.VMEM((UNITS, UNIT_K, UNIT_N), BF),
                pltpu.VMEM((2, slots, ff), F32),
                pltpu.VMEM((tok, dim), BF),
                pltpu.VMEM((slots, dim), BF),
                pltpu.VMEM((slots, ff), BF),
                pltpu.VMEM((2, stack, ff), BF),
                pltpu.VMEM((stack, ff), BF),
                pltpu.VMEM((stack, dim), BF),
                pltpu.VMEM((groups, slab, width + stack), BF),
                pltpu.VMEM((groups, slab, width + stack), BF),
                pltpu.VMEM((k_in - 1, groups, slab, width), BF),
                pltpu.VMEM((k_in - 1, groups, slab, width), BF),
                pltpu.VMEM((n_out, groups, slab, MAIN), BF),
                pltpu.VMEM((slots, stack), F32),
                pltpu.VMEM((2, slots, stack), BF),
                pltpu.VMEM((1 + cap // 2, tok, groups * slab), BF),
                dma((UNITS,)), dma((8,)), dma((k_in, groups)), dma((k_in, groups)), dma((n_out, groups)), dma((n_out, groups)),
            ],
            compiler_params=pltpu.CompilerParams(collective_id=0, has_side_effects=True, vmem_limit_bytes=67043328),
            name="lora_swiglu",
        )(adapter_id.reshape(1, tok), x, w_gate, w_up, w_down, *flat)

    return jax.shard_map(device_step, mesh=mesh, in_specs=(row_spec, id_spec, P(), P(), P(), owned_spec, owned_spec, owned_spec, owned_spec, owned_spec, owned_spec), out_specs=row_spec, check_vma=False)
```

```python
import functools
import math

import jax
import jax.numpy as jnp
from jax import lax
from jax.experimental import pallas as pl
from jax.experimental.pallas import tpu as pltpu
from jax.sharding import PartitionSpec as P

LORA_ALPHA = 32
BF, F32 = jnp.bfloat16, jnp.float32
CORES = 2
UNIT_K, UNIT_N = 1024, 512
UNITS = 32
MAIN = 384


def one_hot(rows, cols, hit):
    r = lax.broadcasted_iota(jnp.int32, (rows, cols), 0)
    c = lax.broadcasted_iota(jnp.int32, (rows, cols), 1)
    return hit(r, c).astype(F32).astype(BF)


def dot(a, b):
    return jnp.dot(a, b, preferred_element_type=F32)


def dot_t(a, b):
    return lax.dot_general(a, b, (((1,), (1,)), ((), ())), preferred_element_type=F32)


def layer(groups, cap, scale, rank, ids_ref, x_hbm, wg_hbm, wu_hbm, wd_hbm, ag_hbm, bg_hbm, au_hbm, bu_hbm, ad_hbm, bd_hbm, out_hbm,
          ring, acc_v, x_v, xc, h_v, bgu, adv, bdv, sendx, recvx, sendm, recvm, land, keep_v, low_v, gmat, unmap, remap,
          ring_sem, in_sem, s1_sem, r1_sem, s2_sem, land_sem):
    tok, dim = x_v.shape
    ff = h_v.shape[1]
    stack = bdv.shape[0]
    slots = groups * cap
    slab = recvm.shape[2]
    packed = groups * slab
    side = math.isqrt(groups // CORES)
    third = cap // 2
    n_in = ff // UNIT_N
    n_out = dim // UNIT_N
    k_out = ff // UNIT_K
    passes = ((0, 1), (1, 1)) + tuple((c, 2) for c in range(2, n_out, 2))
    last_pass = len(passes) - 1
    me = lax.axis_index("data")
    my_c, my_x, my_y = lax.rem(me, CORES), lax.rem(me // CORES, side), me // (CORES * side)

    chips = side * side

    def device(dy, dx, dc):
        return {"data": (lax.rem(my_y + dy % side, side) * side + lax.rem(my_x + dx % side, side)) * CORES + lax.rem(my_c + dc, CORES)}

    def target(r, back=False):
        sign = -1 if back else 1
        return device(sign * (r // (CORES * side)), sign * ((r // CORES) % side), r % CORES)

    def hops(r):
        dy, dx = r // (CORES * side), (r // CORES) % side
        return min(dy, side - dy) + min(dx, side - dx)

    order = sorted(range(1, groups), key=lambda r: -hops(r))

    def remote(src, dst, ssem, rsem, to):
        return pltpu.make_async_remote_copy(src, dst, ssem, rsem, device_id=to, device_id_type=pl.DeviceIdType.MESH)

    per_step = 8

    def in_copy(src, dst, i):
        return pltpu.make_async_copy(src, dst, in_sem.at[i])

    def fill(p, base, unit, slot):
        c, n = passes[p]
        rows = n * UNIT_N
        per = 2 // n
        for part in range(per):
            which = part if per == 2 else unit % 2
            block = (base + unit) if per == 2 else base // 2 + unit // 2
            col = pl.multiple_of(block * UNIT_N, UNIT_N)
            src = (wg_hbm, wu_hbm)[which].at[pl.ds(c * UNIT_N, rows), pl.ds(col, UNIT_N)]
            pltpu.make_async_copy(src, ring.at[slot, pl.ds(part * rows, rows)], ring_sem.at[lax.div(slot, per_step)]).start()

    def filled(slot):
        ref = ring.at[pl.ds(slot, per_step)]
        pltpu.make_async_copy(ref, ref, ring_sem.at[lax.div(slot, per_step)]).wait()

    def out_unit(n, k, slot):
        col = pl.multiple_of(n * UNIT_N, UNIT_N)
        return pltpu.make_async_copy(wd_hbm.at[pl.ds(k * UNIT_K, UNIT_K), pl.ds(col, UNIT_N)], ring.at[slot], ring_sem.at[lax.div(slot, per_step)])

    x_copy = in_copy(x_hbm, x_v, 0)
    x_copy.start()
    early = [in_copy(ag_hbm, h_v.at[pl.ds(0, stack), pl.ds(0, dim)], 1), in_copy(au_hbm, h_v.at[pl.ds(0, stack), pl.ds(dim, dim)], 2),
             in_copy(bg_hbm, bgu.at[0], 3), in_copy(bu_hbm, bgu.at[1], 4)]
    late = [in_copy(ad_hbm, adv, 5), in_copy(bd_hbm, bdv, 6)]

    with jax.named_scope("signal"):
        barrier = pltpu.get_barrier_semaphore()
        for r in range(1, groups):
            pl.semaphore_signal(barrier, inc=1, device_id=target(r), device_id_type=pl.DeviceIdType.MESH)

    with jax.named_scope("place"):
        ids = ids_ref[...].astype(F32)
        eye = lax.broadcasted_iota(jnp.int32, (tok, tok), 0) == lax.broadcasted_iota(jnp.int32, (tok, tok), 1)
        ids_c = jnp.sum(jnp.where(eye, jnp.broadcast_to(ids, (tok, tok)), 0.0), axis=1, keepdims=True)
        per_owner = stack // rank

        def fdiv(v, n):
            return jnp.floor((v + 0.5) * (1.0 / n))

        def place(v):
            owner = fdiv(v, per_owner)
            local = v - owner * per_owner
            oy = fdiv(owner, CORES * side)
            ox = fdiv(owner, CORES) - oy * side
            oc = owner - fdiv(owner, CORES) * CORES

            def mod(a, b, n):
                d = a - b.astype(F32)
                return jnp.where(d < 0, d + n, d)
            rel = (mod(oy, my_y, side) * side + mod(ox, my_x, side)) * CORES + mod(oc, my_c, CORES)
            return owner, local, rel

        own_r, _, rel_r = place(ids)
        own_c, loc_c, rel_c = place(ids_c)
        t0 = lax.broadcasted_iota(jnp.int32, (tok, tok), 0)
        t1 = lax.broadcasted_iota(jnp.int32, (tok, tok), 1)
        same = own_c == own_r
        arr_r = jnp.sum(jnp.where(same & (t0 < t1), 1.0, 0.0), axis=0, keepdims=True)
        arr_c = jnp.sum(jnp.where(same & (t1 < t0), 1.0, 0.0), axis=1, keepdims=True)

        def rows_of(rel, arr):
            main = (rel * slab + arr).astype(jnp.int32)
            tail_row = fdiv(arr, third)
            tail = (rel * slab + cap + tail_row).astype(jnp.int32)
            part = (arr - tail_row * third).astype(jnp.int32)
            return main, tail, part

        main_r, tail_r, part_r = rows_of(rel_r, arr_r)
        main_c, tail_c, part_c = rows_of(rel_c, arr_c)
        s_main = one_hot(packed, tok, lambda r, c: r == main_r)
        s_tail = [one_hot(packed, tok, lambda r, c: (r == tail_r) & (part_r == k)) for k in range(third)]
        gmat[0] = one_hot(tok, packed, lambda r, c: c == main_c)
        for k in range(third):
            gmat[1 + k] = one_hot(tok, packed, lambda r, c: (c == tail_c) & (part_c == k))
        mine = one_hot(tok, stack, lambda r, c: loc_c == fdiv(c.astype(F32), rank))

    with jax.named_scope("x_wait"):
        x_copy.wait()
    with jax.named_scope("weights"):
        for p in range(2):
            for u in range(UNITS // 2):
                fill(p, 0, u, p * (UNITS // 2) + u)
        for c in early + late:
            c.start()

    n_pass = len(passes)

    def copy1(p, r):
        q, dc = r // CORES, r % CORES
        if p == n_pass:
            src, dst = sendm.at[q, dc], recvm.at[q, dc]
        else:
            at = pl.ds(*passes[p])
            src, dst = sendx.at[at, q, dc], recvx.at[at, q, dc]
        near = int(q == 0)
        return remote(src, dst, s1_sem.at[int(p == n_pass), near], r1_sem.at[p, near], target(r))

    others = pl.ds(1, chips - 1)

    def all_of(ref, ssem, rsem):
        return remote(ref, ref, ssem, rsem, target(1))

    for p in range(n_pass + 1):
        with jax.named_scope(f"pack{p}"):
            if p == n_pass:
                sendm[...] = dot(s_main, mine).reshape(chips, CORES, slab, stack).astype(BF)
            else:
                for b in range(passes[p][0], sum(passes[p])):
                    xa = x_v[:, b * UNIT_N:b * UNIT_N + MAIN]
                    xb = x_v[:, b * UNIT_N + MAIN:(b + 1) * UNIT_N]
                    both = dot(s_main, xa) + jnp.concatenate([dot(s, xb) for s in s_tail], axis=1)
                    sendx[b] = both.reshape(chips, CORES, slab, MAIN).astype(BF)
        if p == 0:
            with jax.named_scope("bar_wait"):
                pl.semaphore_wait(barrier, groups - 1)
        with jax.named_scope(f"send{p}"):
            for r in order:
                copy1(p, r).start()
            if p == n_pass:
                recvm[0, 0] = sendm[0, 0]
            else:
                for b in range(passes[p][0], sum(passes[p])):
                    recvx[b, 0, 0] = sendx[b, 0, 0]

    def slot_of(s):
        g = fdiv(s.astype(F32), cap).astype(jnp.int32)
        return g, s - g * cap

    def unpack_main(r, c):
        g, j = slot_of(r)
        return c == g * slab + j

    def unpack_tail(k):
        def hit(r, c):
            g, j = slot_of(r)
            q = fdiv(j.astype(F32), third).astype(jnp.int32)
            return (c == g * slab + cap + q) & (j - q * third == k)
        return hit

    def pack_main(r, c):
        return unpack_main(c, r)

    def pack_tail(k):
        def hit(r, c):
            return unpack_tail(k)(c, r)
        return hit

    with jax.named_scope("maps"):
        unmap[0] = one_hot(slots, packed, unpack_main)
        remap[0] = one_hot(packed, slots, pack_main)
        for k in range(third):
            unmap[1 + k] = one_hot(slots, packed, unpack_tail(k))
            remap[1 + k] = one_hot(packed, slots, pack_tail(k))
    w = MAIN // third

    def dense(v):
        return v.astype(F32).reshape(packed, v.shape[-1]).astype(BF)

    def arrive(p):
        with jax.named_scope(f"recv{p}"):
            if p == n_pass:
                all_of(recvm.at[others], s1_sem.at[1, 0], r1_sem.at[p, 0]).wait_recv()
                all_of(recvm.at[0, 1], s1_sem.at[1, 1], r1_sem.at[p, 1]).wait_recv()
            else:
                at = pl.ds(*passes[p])
                all_of(recvx.at[at, others], s1_sem.at[0, 0], r1_sem.at[p, 0]).wait_recv()
                all_of(recvx.at[at, 0, 1], s1_sem.at[0, 1], r1_sem.at[p, 1]).wait_recv()
        with jax.named_scope(f"unpack{p}"):
            if p == n_pass:
                keep_v[...] = dot(unmap[0], dense(recvm[...]))
            else:
                for b in range(passes[p][0], sum(passes[p])):
                    part = dense(recvx[b])
                    xc[:, b * UNIT_N:b * UNIT_N + MAIN] = dot(unmap[0], part).astype(BF)
                    tail = sum(dot(unmap[1 + k], part[:, k * w:(k + 1) * w]) for k in range(third))
                    xc[:, b * UNIT_N + MAIN:(b + 1) * UNIT_N] = tail.astype(BF)

    def pick(low):
        return jnp.where(keep_v[...] > 0.5, low.astype(BF).astype(F32), 0.0).astype(BF)

    for p in range(n_pass):
        arrive(p)
        c, n = passes[p]
        rows = n * UNIT_N
        if p == last_pass:
            arrive(n_pass)
            with jax.named_scope("low"):
                for cp in early:
                    cp.wait()
                for i in range(2):
                    low_v[i] = pick(sum(dot_t(xc[:, k:k + UNIT_N], h_v[0:stack, i * dim + k:i * dim + k + UNIT_N]) for k in range(0, dim, UNIT_N)))
        start = p * (UNITS // 2) if n == 1 else 0
        blocks = per_step if n == 1 else per_step // 2

        def step(i, carry):
            base = i * per_step
            filled(pl.multiple_of(start + base, per_step))
            with jax.named_scope(f"dot{p}"):
                for b in range(blocks):
                    for s in range(UNIT_N // 256):
                        col = pl.ds(pl.multiple_of((i * blocks + b) * UNIT_N + s * 256, 256), 256)
                        res = []
                        for which in range(2):
                            slot, row = (start + base + b, which * rows) if n == 1 else (base + b * 2 + which, 0)
                            d = dot(xc[:, c * UNIT_N:c * UNIT_N + rows], ring[slot, row:row + rows, s * 256:(s + 1) * 256])
                            if p > 0:
                                d = acc_v[which, :, col] + d
                            if p < last_pass:
                                acc_v[which, :, col] = d
                            else:
                                res.append(d + (scale * dot(low_v[which], bgu[which, :, col])).astype(BF).astype(F32))
                        if res:
                            g, u = res
                            h_v[:, col] = (g * (1.0 / (1.0 + jnp.exp(-g))) * u).astype(BF)
            for k in range(per_step):
                slot = start + base + k
                if p == last_pass:
                    out_unit(i, k, slot).start()
                elif p == 0:
                    fill(2, base, k, slot)
                elif p == 1:
                    fill(2, base + UNITS // 2, k, slot)
                else:
                    fill(p + 1, base, k, slot)
            return carry

        lax.fori_loop(0, (UNITS // 2 if n == 1 else UNITS) // per_step, step, 0)

    with jax.named_scope("low2"):
        for cp in late:
            cp.wait()
        @pl.when(me >= 0)
        def _():
            low_v[0] = pick(sum(dot_t(h_v[:, k:k + UNIT_K], adv[:, k:k + UNIT_K]) for k in range(0, ff, UNIT_K)))
    all_of(sendx.at[:, others], s1_sem.at[0, 0], r1_sem.at[0, 0]).wait_send()
    all_of(sendx.at[:, 0, 1], s1_sem.at[0, 1], r1_sem.at[0, 1]).wait_send()
    all_of(sendm.at[others], s1_sem.at[1, 0], r1_sem.at[0, 0]).wait_send()
    all_of(sendm.at[0, 1], s1_sem.at[1, 1], r1_sem.at[0, 1]).wait_send()

    def ship(n):
        with jax.named_scope(f"ship{n}"):
            for r in order:
                q, dc = r // CORES, r % CORES
                near = int(q == 0)
                remote(sendx.at[n, q, dc], land.at[n, q, dc], s2_sem.at[near], land_sem.at[n, near], target(r, True)).start()

    def home(n):
        with jax.named_scope(f"homewait{n}"):
            all_of(land.at[n, others], s2_sem.at[0], land_sem.at[n, 0]).wait_recv()
            all_of(land.at[n, 0, 1], s2_sem.at[1], land_sem.at[n, 1]).wait_recv()
        with jax.named_scope(f"home{n}"):
            part = dense(land[n])
            x_v[:, n * UNIT_N:n * UNIT_N + MAIN] = dot(gmat[0], part).astype(BF)
            tail = sum(dot(gmat[1 + k], part[:, k * w:(k + 1) * w]) for k in range(third))
            x_v[:, n * UNIT_N + MAIN:(n + 1) * UNIT_N] = tail.astype(BF)

    for n in range(n_out):
        base = n * k_out
        filled(base % UNITS)
        if n > 0:
            ship(n - 1)
        with jax.named_scope(f"out{n}"):
            done = []
            for s in range(UNIT_N // 256):
                cols = slice(n * UNIT_N + s * 256, n * UNIT_N + (s + 1) * 256)
                acc = None
                for k in range(k_out):
                    d = dot(h_v[:, k * UNIT_K:(k + 1) * UNIT_K], ring[(base + k) % UNITS, :, s * 256:(s + 1) * 256])
                    acc = d if acc is None else acc + d
                delta = (scale * dot(low_v[0], bdv[:, cols])).astype(BF).astype(F32)
                done.append((xc[:, cols].astype(F32) + (acc + delta)).astype(BF))
            done = jnp.concatenate(done, axis=1)
            both = dot(remap[0], done[:, :MAIN]) + jnp.concatenate([dot(remap[1 + k], done[:, MAIN:]) for k in range(third)], axis=1)
            sendx[n] = both.reshape(chips, CORES, slab, MAIN).astype(BF)
            land[n, 0, 0] = sendx[n, 0, 0]
        ahead = n + UNITS // k_out
        for k in range(k_out):
            if ahead < n_out:
                out_unit(ahead, k, (base + k) % UNITS).start()
        if n > 2:
            home(n - 3)
    ship(n_out - 1)
    for n in range(n_out - 3, n_out):
        home(n)
    all_of(sendx.at[:, others], s2_sem.at[0], land_sem.at[0, 0]).wait_send()
    all_of(sendx.at[:, 0, 1], s2_sem.at[1], land_sem.at[0, 1]).wait_send()
    last = in_copy(x_v, out_hbm, 7)
    last.start()
    last.wait()


def solution(mesh):
    groups = mesh.shape["data"]
    row_spec = P(("rep", "data"), None)
    id_spec = P(("rep", "data"))
    owned_spec = P("data", None, None)

    def device_step(x, adapter_id, w_gate, w_up, w_down, a_gate, b_gate, a_up, b_up, a_down, b_down):
        tok, dim = x.shape
        ff = w_gate.shape[1]
        per_owner, rank, _ = a_gate.shape
        stack = per_owner * rank
        cap = (3 * tok + groups - 1) // groups
        slots = groups * cap
        slab = 8
        n_out = dim // UNIT_N
        chips = groups // CORES
        flat = [m.reshape(stack, m.shape[2]) for m in (a_gate, b_gate, a_up, b_up, a_down, b_down)]
        anyspec = pl.BlockSpec(memory_space=pl.ANY)
        dma = pltpu.SemaphoreType.DMA
        return pl.pallas_call(
            functools.partial(layer, groups, cap, LORA_ALPHA / rank, rank),
            out_shape=jax.ShapeDtypeStruct((tok, dim), BF),
            in_specs=[pl.BlockSpec(memory_space=pltpu.VMEM)] + [anyspec] * 10,
            out_specs=anyspec,
            scratch_shapes=[
                pltpu.VMEM((UNITS, UNIT_K, UNIT_N), BF),
                pltpu.VMEM((2, slots, ff), F32),
                pltpu.VMEM((tok, dim), BF),
                pltpu.VMEM((slots, dim), BF),
                pltpu.VMEM((slots, ff), BF),
                pltpu.VMEM((2, stack, ff), BF),
                pltpu.VMEM((stack, ff), BF),
                pltpu.VMEM((stack, dim), BF),
                pltpu.VMEM((n_out, chips, CORES, slab, MAIN), BF),
                pltpu.VMEM((n_out, chips, CORES, slab, MAIN), BF),
                pltpu.VMEM((chips, CORES, slab, stack), BF),
                pltpu.VMEM((chips, CORES, slab, stack), BF),
                pltpu.VMEM((n_out, chips, CORES, slab, MAIN), BF),
                pltpu.VMEM((slots, stack), F32),
                pltpu.VMEM((2, slots, stack), BF),
                pltpu.VMEM((1 + cap // 2, tok, groups * slab), BF),
                pltpu.VMEM((1 + cap // 2, slots, groups * slab), BF),
                pltpu.VMEM((1 + cap // 2, groups * slab, slots), BF),
                dma((UNITS // 8,)), dma((8,)), dma((2, 2)), dma((n_out, 2)), dma((2,)), dma((n_out, 2)),
            ],
            compiler_params=pltpu.CompilerParams(collective_id=0, has_side_effects=True, vmem_limit_bytes=67043328),
            name="lora_swiglu",
        )(adapter_id.reshape(1, tok), x, w_gate, w_up, w_down, *flat)

    return jax.shard_map(device_step, mesh=mesh, in_specs=(row_spec, id_spec, P(), P(), P(), owned_spec, owned_spec, owned_spec, owned_spec, owned_spec, owned_spec), out_specs=row_spec, check_vma=False)
```

```python
import functools
import math

import jax
import jax.numpy as jnp
from jax import lax
from jax.experimental import pallas as pl
from jax.experimental.pallas import tpu as pltpu
from jax.sharding import PartitionSpec as P

LORA_ALPHA = 32
BF, F32 = jnp.bfloat16, jnp.float32
CORES = 2
UNIT_K, UNIT_N = 1024, 512
UNITS = 32
GROUPS = 2
MAIN = 384


def one_hot(rows, cols, hit):
    r = lax.broadcasted_iota(jnp.int32, (rows, cols), 0)
    c = lax.broadcasted_iota(jnp.int32, (rows, cols), 1)
    return hit(r, c).astype(F32).astype(BF)


def dot(a, b):
    return jnp.dot(a, b, preferred_element_type=F32)


def dot_t(a, b):
    return lax.dot_general(a, b, (((1,), (1,)), ((), ())), preferred_element_type=F32)


def layer(groups, cap, scale, rank, ids_ref, x_hbm, wg_hbm, wu_hbm, wd_hbm, ag_hbm, bg_hbm, au_hbm, bu_hbm, ad_hbm, bd_hbm, out_v,
          ring, acc_v, x_v, xc, h_v, bgu, adv, bdv, sendx, recvx, sendm, recvm, land, keep_v, low_v, gmat, unmap, remap,
          ring_sem, in_sem, s1_sem, r1_sem, s2_sem, land_sem, part_sem, free_sem):
    tok, dim = x_v.shape
    ff = h_v.shape[1]
    stack = bdv.shape[0]
    slots = groups * cap
    slab = recvm.shape[2]
    packed = groups * slab
    side = math.isqrt(groups // CORES)
    third = cap // 2
    n_in = ff // UNIT_N
    n_out = dim // UNIT_N
    k_out = ff // UNIT_K
    passes = ((0, 1), (1, 1)) + tuple((c, 2) for c in range(2, n_out, 2))
    last_pass = len(passes) - 1
    me = lax.axis_index("data")
    my_c, my_x, my_y = lax.rem(me, CORES), lax.rem(me // CORES, side), me // (CORES * side)

    chips = side * side

    def device(dy, dx, dc):
        return {"data": (lax.rem(my_y + dy % side, side) * side + lax.rem(my_x + dx % side, side)) * CORES + lax.rem(my_c + dc, CORES)}

    def target(r, back=False):
        sign = -1 if back else 1
        return device(sign * (r // (CORES * side)), sign * ((r // CORES) % side), r % CORES)

    def hops(r):
        dy, dx = r // (CORES * side), (r // CORES) % side
        return min(dy, side - dy) + min(dx, side - dx)

    order = sorted(range(1, groups), key=lambda r: -hops(r))

    def remote(src, dst, ssem, rsem, to):
        return pltpu.make_async_remote_copy(src, dst, ssem, rsem, device_id=to, device_id_type=pl.DeviceIdType.MESH)

    per_step = 8

    def in_copy(src, dst, i):
        return pltpu.make_async_copy(src, dst, in_sem.at[i])

    def fill(p, base, unit, slot):
        c, n = passes[p]
        rows = n * UNIT_N
        per = 2 // n
        for part in range(per):
            which = part if per == 2 else unit % 2
            block = (base + unit) if per == 2 else base // 2 + unit // 2
            col = pl.multiple_of(block * UNIT_N, UNIT_N)
            src = (wg_hbm, wu_hbm)[which].at[pl.ds(c * UNIT_N, rows), pl.ds(col, UNIT_N)]
            pltpu.make_async_copy(src, ring.at[slot, pl.ds(part * rows, rows)], ring_sem.at[lax.div(slot, per_step)]).start()

    def filled(slot):
        ref = ring.at[pl.ds(slot, per_step)]
        pltpu.make_async_copy(ref, ref, ring_sem.at[lax.div(slot, per_step)]).wait()

    def out_unit(n, k, slot):
        col = pl.multiple_of(n * UNIT_N, UNIT_N)
        return pltpu.make_async_copy(wd_hbm.at[pl.ds(k * UNIT_K, UNIT_K), pl.ds(col, UNIT_N)], ring.at[slot], ring_sem.at[lax.div(slot, per_step)])

    x_copy = in_copy(x_hbm, x_v, 0)
    x_copy.start()
    with jax.named_scope("signal"):
        barrier = pltpu.get_barrier_semaphore()
        for r in order:
            pl.semaphore_signal(barrier, inc=1, device_id=target(r), device_id_type=pl.DeviceIdType.MESH)

    early = [in_copy(ag_hbm, h_v.at[pl.ds(0, stack), pl.ds(0, dim)], 1), in_copy(au_hbm, h_v.at[pl.ds(0, stack), pl.ds(dim, dim)], 2),
             in_copy(bg_hbm, bgu.at[0], 3), in_copy(bu_hbm, bgu.at[1], 4)]
    late = [in_copy(ad_hbm, adv, 5), in_copy(bd_hbm, bdv, 6)]

    with jax.named_scope("place"):
        ids = ids_ref[...].astype(F32)
        eye = lax.broadcasted_iota(jnp.int32, (tok, tok), 0) == lax.broadcasted_iota(jnp.int32, (tok, tok), 1)
        ids_c = jnp.sum(jnp.where(eye, jnp.broadcast_to(ids, (tok, tok)), 0.0), axis=1, keepdims=True)
        per_owner = stack // rank

        def fdiv(v, n):
            return jnp.floor((v + 0.5) * (1.0 / n))

        def place(v):
            owner = fdiv(v, per_owner)
            local = v - owner * per_owner
            oy = fdiv(owner, CORES * side)
            ox = fdiv(owner, CORES) - oy * side
            oc = owner - fdiv(owner, CORES) * CORES

            def mod(a, b, n):
                d = a - b.astype(F32)
                return jnp.where(d < 0, d + n, d)
            rel = (mod(oy, my_y, side) * side + mod(ox, my_x, side)) * CORES + mod(oc, my_c, CORES)
            return owner, local, rel

        own_r, _, rel_r = place(ids)
        own_c, loc_c, rel_c = place(ids_c)
        t0 = lax.broadcasted_iota(jnp.int32, (tok, tok), 0)
        t1 = lax.broadcasted_iota(jnp.int32, (tok, tok), 1)
        same = own_c == own_r
        arr_r = jnp.sum(jnp.where(same & (t0 < t1), 1.0, 0.0), axis=0, keepdims=True)
        arr_c = jnp.sum(jnp.where(same & (t1 < t0), 1.0, 0.0), axis=1, keepdims=True)

        def rows_of(rel, arr):
            main = (rel * slab + arr).astype(jnp.int32)
            tail_row = fdiv(arr, third)
            tail = (rel * slab + cap + tail_row).astype(jnp.int32)
            part = (arr - tail_row * third).astype(jnp.int32)
            return main, tail, part

        main_r, tail_r, part_r = rows_of(rel_r, arr_r)
        main_c, tail_c, part_c = rows_of(rel_c, arr_c)
        s_main = one_hot(packed, tok, lambda r, c: r == main_r)
        s_tail = [one_hot(packed, tok, lambda r, c: (r == tail_r) & (part_r == k)) for k in range(third)]
        gmat[0] = one_hot(tok, packed, lambda r, c: c == main_c)
        for k in range(third):
            gmat[1 + k] = one_hot(tok, packed, lambda r, c: (c == tail_c) & (part_c == k))
        mine = one_hot(tok, stack, lambda r, c: loc_c == fdiv(c.astype(F32), rank))

    with jax.named_scope("x_wait"):
        x_copy.wait()
    with jax.named_scope("weights"):
        for p in range(2):
            for u in range(UNITS // 2):
                fill(p, 0, u, p * (UNITS // 2) + u)

    n_pass = len(passes)

    def copy1(p, r):
        q, dc = r // CORES, r % CORES
        if p == n_pass:
            src, dst = sendm.at[q, dc], recvm.at[q, dc]
        else:
            at = pl.ds(*passes[p])
            src, dst = sendx.at[at, q, dc], recvx.at[at, q, dc]
        near = int(q == 0)
        return remote(src, dst, s1_sem.at[int(p == n_pass), near], r1_sem.at[p, near], target(r))

    others = pl.ds(1, chips - 1)

    def all_of(ref, ssem, rsem):
        return remote(ref, ref, ssem, rsem, target(1))

    for p in range(n_pass + 1):
        with jax.named_scope(f"pack{p}"):
            if p == n_pass:
                sendm[...] = dot(s_main, mine).reshape(chips, CORES, slab, stack).astype(BF)
            else:
                for b in range(passes[p][0], sum(passes[p])):
                    xa = x_v[:, b * UNIT_N:b * UNIT_N + MAIN]
                    xb = x_v[:, b * UNIT_N + MAIN:(b + 1) * UNIT_N]
                    both = dot(s_main, xa) + jnp.concatenate([dot(s, xb) for s in s_tail], axis=1)
                    sendx[b] = both.reshape(chips, CORES, slab, MAIN).astype(BF)
        if p == 0:
            with jax.named_scope("bar_wait"):
                pl.semaphore_wait(barrier, groups - 1)
        with jax.named_scope(f"send{p}"):
            for r in order:
                copy1(p, r).start()
            if p == n_pass:
                recvm[0, 0] = sendm[0, 0]
            else:
                for b in range(passes[p][0], sum(passes[p])):
                    recvx[b, 0, 0] = sendx[b, 0, 0]

    def slot_of(s):
        g = fdiv(s.astype(F32), cap).astype(jnp.int32)
        return g, s - g * cap

    def unpack_main(r, c):
        g, j = slot_of(r)
        return c == g * slab + j

    def unpack_tail(k):
        def hit(r, c):
            g, j = slot_of(r)
            q = fdiv(j.astype(F32), third).astype(jnp.int32)
            return (c == g * slab + cap + q) & (j - q * third == k)
        return hit

    def pack_main(r, c):
        return unpack_main(c, r)

    def pack_tail(k):
        def hit(r, c):
            return unpack_tail(k)(c, r)
        return hit

    with jax.named_scope("maps"):
        unmap[0] = one_hot(slots, packed, unpack_main)
        remap[0] = one_hot(packed, slots, pack_main)
        for k in range(third):
            unmap[1 + k] = one_hot(slots, packed, unpack_tail(k))
            remap[1 + k] = one_hot(packed, slots, pack_tail(k))
    w = MAIN // third

    def dense(v):
        return v.astype(F32).reshape(packed, v.shape[-1]).astype(BF)

    def arrive(p):
        with jax.named_scope(f"recv{p}"):
            if p == n_pass:
                all_of(recvm.at[others], s1_sem.at[1, 0], r1_sem.at[p, 0]).wait_recv()
                all_of(recvm.at[0, 1], s1_sem.at[1, 1], r1_sem.at[p, 1]).wait_recv()
            else:
                at = pl.ds(*passes[p])
                all_of(recvx.at[at, others], s1_sem.at[0, 0], r1_sem.at[p, 0]).wait_recv()
                all_of(recvx.at[at, 0, 1], s1_sem.at[0, 1], r1_sem.at[p, 1]).wait_recv()
        with jax.named_scope(f"unpack{p}"):
            if p == n_pass:
                keep_v[...] = dot(unmap[0], dense(recvm[...]))
            else:
                for b in range(passes[p][0], sum(passes[p])):
                    part = dense(recvx[b])
                    xc[:, b * UNIT_N:b * UNIT_N + MAIN] = dot(unmap[0], part).astype(BF)
                    tail = sum(dot(unmap[1 + k], part[:, k * w:(k + 1) * w]) for k in range(third))
                    xc[:, b * UNIT_N + MAIN:(b + 1) * UNIT_N] = tail.astype(BF)

    def pick(low):
        return jnp.where(keep_v[...] > 0.5, low.astype(BF).astype(F32), 0.0).astype(BF)

    for p in range(n_pass):
        arrive(p)
        c, n = passes[p]
        rows = n * UNIT_N
        if p == last_pass:
            arrive(n_pass)
            pl.semaphore_signal(free_sem, inc=1, device_id=device(0, 0, 1), device_id_type=pl.DeviceIdType.MESH)
            with jax.named_scope("low"):
                for cp in early:
                    cp.wait()
                for i in range(2):
                    low_v[i] = pick(sum(dot_t(xc[:, k:k + UNIT_N], h_v[0:stack, i * dim + k:i * dim + k + UNIT_N]) for k in range(0, dim, UNIT_N)))
        start = p * (UNITS // 2) if n == 1 else 0
        size = (GROUPS if n == 1 else 1) * per_step
        blocks = size if n == 1 else size // 2

        def step(i, carry):
            base = i * size
            if n == 1:
                for g in range(GROUPS):
                    filled(start + base + g * per_step)
            with jax.named_scope(f"dot{p}"):
                for b in range(blocks):
                    if n > 1 and b * size // blocks % per_step == 0:
                        filled(start + base + b * size // blocks)
                    for s in range(UNIT_N // 256):
                        col = pl.ds(pl.multiple_of((i * blocks + b) * UNIT_N + s * 256, 256), 256)
                        res = []
                        for which in range(2):
                            slot, row = (start + base + b, which * rows) if n == 1 else (base + b * 2 + which, 0)
                            d = dot(xc[:, c * UNIT_N:c * UNIT_N + rows], ring[slot, row:row + rows, s * 256:(s + 1) * 256])
                            if p > 0:
                                d = acc_v[which, :, col] + d
                            if p < last_pass:
                                acc_v[which, :, col] = d
                            else:
                                res.append(d + (scale * dot(low_v[which], bgu[which, :, col])).astype(BF).astype(F32))
                        if res:
                            g, u = res
                            h_v[:, col] = (g * (1.0 / (1.0 + jnp.exp(-g))) * u).astype(BF)
                    if (b + 1) * size // blocks % per_step:
                        continue
                    for k in range((b + 1) * size // blocks - per_step, (b + 1) * size // blocks):
                        slot = start + base + k
                        if p == last_pass:
                            out_unit(i * size // per_step + k // per_step, k % per_step, slot).start()
                        elif p == 0:
                            fill(2, base, k, slot)
                        elif p == 1:
                            fill(2, base + UNITS // 2, k, slot)
                        else:
                            fill(p + 1, base, k, slot)
            return carry

        steps = (UNITS // 2 if n == 1 else UNITS) // size
        if p == last_pass:
            for cp in late:
                cp.start()
        if steps == 1:
            step(0, 0)
        else:
            lax.fori_loop(0, steps, step, 0)
        if p == 1:
            for cp in early:
                cp.start()

    with jax.named_scope("low2"):
        for cp in late:
            cp.wait()
        @pl.when(me >= 0)
        def _():
            low_v[0] = pick(sum(dot_t(h_v[:, k:k + UNIT_K], adv[:, k:k + UNIT_K]) for k in range(0, ff, UNIT_K)))
    all_of(sendx.at[:, others], s1_sem.at[0, 0], r1_sem.at[0, 0]).wait_send()
    all_of(sendx.at[:, 0, 1], s1_sem.at[0, 1], r1_sem.at[0, 1]).wait_send()
    all_of(sendm.at[others], s1_sem.at[1, 0], r1_sem.at[0, 0]).wait_send()
    all_of(sendm.at[0, 1], s1_sem.at[1, 1], r1_sem.at[0, 1]).wait_send()

    def ship(n):
        with jax.named_scope(f"ship{n}"):
            for r in order:
                q, dc = r // CORES, r % CORES
                near = int(q == 0)
                remote(sendx.at[n, q, dc], land.at[n, q, dc], s2_sem.at[near], land_sem.at[n, near], target(r, True)).start()

    chip_order = [r // CORES for r in order if r % CORES == 0]

    def ship_pairs(n):
        with jax.named_scope(f"shipp{n}"):
            for q in chip_order:
                remote(sendx.at[n, q], land.at[n, q], s2_sem.at[2], land_sem.at[n, 0], target(q * CORES, True)).start()

    def hand_on(n):
        with jax.named_scope(f"hand{n}"):
            all_of(land.at[n, others], s2_sem.at[2], land_sem.at[n, 0]).wait_recv()
            if n == 0:
                pl.semaphore_wait(free_sem, 1)
            remote(land.at[n, :, 1], recvx.at[n, :, 1], s2_sem.at[3], part_sem.at[n], device(0, 0, 1)).start()

    def home(n):
        with jax.named_scope(f"homewait{n}"):
            if n < n_out - 1:
                all_of(recvx.at[n, :, 1], s2_sem.at[3], part_sem.at[n]).wait_recv()
                slabs = jnp.concatenate([land[n, :, 0:1], recvx[n, :, 1:2]], axis=1)
            else:
                all_of(land.at[n, others], s2_sem.at[0], land_sem.at[n, 0]).wait_recv()
                all_of(land.at[n, 0, 1], s2_sem.at[1], land_sem.at[n, 1]).wait_recv()
                slabs = land[n]
        with jax.named_scope(f"home{n}"):
            part = dense(slabs)
            out_v[:, n * UNIT_N:n * UNIT_N + MAIN] = dot(gmat[0], part).astype(BF)
            tail = sum(dot(gmat[1 + k], part[:, k * w:(k + 1) * w]) for k in range(third))
            out_v[:, n * UNIT_N + MAIN:(n + 1) * UNIT_N] = tail.astype(BF)

    for n in range(n_out):
        base = n * k_out
        filled(base % UNITS)
        if n > 0:
            ship_pairs(n - 1)
        if n > 3:
            hand_on(n - 4)
        with jax.named_scope(f"out{n}"):
            done = []
            for s in range(UNIT_N // 256):
                cols = slice(n * UNIT_N + s * 256, n * UNIT_N + (s + 1) * 256)
                acc = None
                for k in range(k_out):
                    d = dot(h_v[:, k * UNIT_K:(k + 1) * UNIT_K], ring[(base + k) % UNITS, :, s * 256:(s + 1) * 256])
                    acc = d if acc is None else acc + d
                delta = (scale * dot(low_v[0], bdv[:, cols])).astype(BF).astype(F32)
                done.append((xc[:, cols].astype(F32) + (acc + delta)).astype(BF))
            done = jnp.concatenate(done, axis=1)
            both = dot(remap[0], done[:, :MAIN]) + jnp.concatenate([dot(remap[1 + k], done[:, MAIN:]) for k in range(third)], axis=1)
            sendx[n] = both.reshape(chips, CORES, slab, MAIN).astype(BF)
            if n < n_out - 1:
                land[n, 0] = sendx[n, 0]
            else:
                land[n, 0, 0] = sendx[n, 0, 0]
        ahead = n + UNITS // k_out
        for k in range(k_out):
            if ahead < n_out:
                out_unit(ahead, k, (base + k) % UNITS).start()
    m = n_out - 1
    ship(m)
    for n in range(m - 3, m):
        hand_on(n)
    for n in range(n_out):
        home(n)
    all_of(sendx.at[m, others], s2_sem.at[0], land_sem.at[0, 0]).wait_send()
    all_of(sendx.at[m, 0, 1], s2_sem.at[1], land_sem.at[0, 1]).wait_send()
    all_of(sendx.at[pl.ds(0, m), others], s2_sem.at[2], land_sem.at[0, 0]).wait_send()
    all_of(land.at[pl.ds(0, m), :, 1], s2_sem.at[3], part_sem.at[0]).wait_send()


def solution(mesh):
    groups = mesh.shape["data"]
    row_spec = P(("rep", "data"), None)
    id_spec = P(("rep", "data"))
    owned_spec = P("data", None, None)

    def device_step(x, adapter_id, w_gate, w_up, w_down, a_gate, b_gate, a_up, b_up, a_down, b_down):
        tok, dim = x.shape
        ff = w_gate.shape[1]
        per_owner, rank, _ = a_gate.shape
        stack = per_owner * rank
        cap = (3 * tok + groups - 1) // groups
        slots = groups * cap
        slab = 8
        n_out = dim // UNIT_N
        chips = groups // CORES
        flat = [m.reshape(stack, m.shape[2]) for m in (a_gate, b_gate, a_up, b_up, a_down, b_down)]
        anyspec = pl.BlockSpec(memory_space=pl.ANY)
        dma = pltpu.SemaphoreType.DMA
        return pl.pallas_call(
            functools.partial(layer, groups, cap, LORA_ALPHA / rank, rank),
            out_shape=jax.ShapeDtypeStruct((tok, dim), BF),
            in_specs=[pl.BlockSpec(memory_space=pltpu.VMEM)] + [anyspec] * 10,
            out_specs=pl.BlockSpec(memory_space=pltpu.VMEM),
            scratch_shapes=[
                pltpu.VMEM((UNITS, UNIT_K, UNIT_N), BF),
                pltpu.VMEM((2, slots, ff), F32),
                pltpu.VMEM((tok, dim), BF),
                pltpu.VMEM((slots, dim), BF),
                pltpu.VMEM((slots, ff), BF),
                pltpu.VMEM((2, stack, ff), BF),
                pltpu.VMEM((stack, ff), BF),
                pltpu.VMEM((stack, dim), BF),
                pltpu.VMEM((n_out, chips, CORES, slab, MAIN), BF),
                pltpu.VMEM((n_out, chips, CORES, slab, MAIN), BF),
                pltpu.VMEM((chips, CORES, slab, stack), BF),
                pltpu.VMEM((chips, CORES, slab, stack), BF),
                pltpu.VMEM((n_out, chips, CORES, slab, MAIN), BF),
                pltpu.VMEM((slots, stack), F32),
                pltpu.VMEM((2, slots, stack), BF),
                pltpu.VMEM((1 + cap // 2, tok, groups * slab), BF),
                pltpu.VMEM((1 + cap // 2, slots, groups * slab), BF),
                pltpu.VMEM((1 + cap // 2, groups * slab, slots), BF),
                dma((UNITS // 8,)), dma((8,)), dma((2, 2)), dma((n_out, 2)), dma((4,)), dma((n_out, 2)), dma((n_out - 1,)), pltpu.SemaphoreType.REGULAR,
            ],
            compiler_params=pltpu.CompilerParams(collective_id=0, has_side_effects=True, vmem_limit_bytes=67043328),
            name="lora_swiglu",
        )(adapter_id.reshape(1, tok), x, w_gate, w_up, w_down, *flat)

    return jax.shard_map(device_step, mesh=mesh, in_specs=(row_spec, id_spec, P(), P(), P(), owned_spec, owned_spec, owned_spec, owned_spec, owned_spec, owned_spec), out_specs=row_spec, check_vma=False)
```

```python
import functools
import math

import jax
import jax.numpy as jnp
from jax import lax
from jax.experimental import pallas as pl
from jax.experimental.pallas import tpu as pltpu
from jax.sharding import PartitionSpec as P

LORA_ALPHA = 32
BF, F32 = jnp.bfloat16, jnp.float32
CORES = 2
UNIT_K, UNIT_N = 1024, 512
UNITS = 32
GROUPS = 2
MAIN = 384


def one_hot(rows, cols, hit):
    r = lax.broadcasted_iota(jnp.int32, (rows, cols), 0)
    c = lax.broadcasted_iota(jnp.int32, (rows, cols), 1)
    return hit(r, c).astype(F32).astype(BF)


def dot(a, b):
    return jnp.dot(a, b, preferred_element_type=F32)


def dot_t(a, b):
    return lax.dot_general(a, b, (((1,), (1,)), ((), ())), preferred_element_type=F32)


def layer(groups, cap, scale, rank, ids_ref, x_hbm, wg_hbm, wu_hbm, wd_hbm, ag_hbm, bg_hbm, au_hbm, bu_hbm, ad_hbm, bd_hbm, out_hbm,
          ring, acc_v, x_v, xc, h_v, bgu, adv, bdv, sendx, recvx, sendm, recvm, land, keep_v, low_v, gmat, unmap, remap,
          ring_sem, in_sem, s1_sem, r1_sem, s2_sem, land_sem, part_sem, free_sem):
    tok, dim = x_v.shape
    ff = h_v.shape[1]
    stack = bdv.shape[0]
    slots = groups * cap
    slab = recvm.shape[2]
    packed = groups * slab
    side = math.isqrt(groups // CORES)
    third = cap // 2
    n_in = ff // UNIT_N
    n_out = dim // UNIT_N
    k_out = ff // UNIT_K
    passes = ((0, 1), (1, 1)) + tuple((c, 2) for c in range(2, n_out, 2))
    last_pass = len(passes) - 1
    me = lax.axis_index("data")
    my_c, my_x, my_y = lax.rem(me, CORES), lax.rem(me // CORES, side), me // (CORES * side)

    chips = side * side

    def device(dy, dx, dc):
        return {"data": (lax.rem(my_y + dy % side, side) * side + lax.rem(my_x + dx % side, side)) * CORES + lax.rem(my_c + dc, CORES)}

    def target(r, back=False):
        sign = -1 if back else 1
        return device(sign * (r // (CORES * side)), sign * ((r // CORES) % side), r % CORES)

    def hops(r):
        dy, dx = r // (CORES * side), (r // CORES) % side
        return min(dy, side - dy) + min(dx, side - dx)

    order = sorted(range(1, groups), key=lambda r: -hops(r))

    def remote(src, dst, ssem, rsem, to):
        return pltpu.make_async_remote_copy(src, dst, ssem, rsem, device_id=to, device_id_type=pl.DeviceIdType.MESH)

    per_step = 8

    def in_copy(src, dst, i):
        return pltpu.make_async_copy(src, dst, in_sem.at[i])

    def fill(p, base, unit, slot):
        c, n = passes[p]
        rows = n * UNIT_N
        per = 2 // n
        for part in range(per):
            which = part if per == 2 else unit % 2
            block = (base + unit) if per == 2 else base // 2 + unit // 2
            col = pl.multiple_of(block * UNIT_N, UNIT_N)
            src = (wg_hbm, wu_hbm)[which].at[pl.ds(c * UNIT_N, rows), pl.ds(col, UNIT_N)]
            pltpu.make_async_copy(src, ring.at[slot, pl.ds(part * rows, rows)], ring_sem.at[lax.div(slot, per_step)]).start()

    def filled(slot):
        ref = ring.at[pl.ds(slot, per_step)]
        pltpu.make_async_copy(ref, ref, ring_sem.at[lax.div(slot, per_step)]).wait()

    def out_unit(n, k, slot):
        col = pl.multiple_of(n * UNIT_N, UNIT_N)
        return pltpu.make_async_copy(wd_hbm.at[pl.ds(k * UNIT_K, UNIT_K), pl.ds(col, UNIT_N)], ring.at[slot], ring_sem.at[lax.div(slot, per_step)])

    x_copy = in_copy(x_hbm, x_v, 0)
    x_copy.start()
    with jax.named_scope("signal"):
        barrier = pltpu.get_barrier_semaphore()
        for r in order:
            pl.semaphore_signal(barrier, inc=1, device_id=target(r), device_id_type=pl.DeviceIdType.MESH)

    early = [in_copy(ag_hbm, h_v.at[pl.ds(0, stack), pl.ds(0, dim)], 1), in_copy(au_hbm, h_v.at[pl.ds(0, stack), pl.ds(dim, dim)], 1),
             in_copy(bg_hbm, bgu.at[0], 2), in_copy(bu_hbm, bgu.at[1], 2)]
    late = [in_copy(ad_hbm, adv, 3), in_copy(bd_hbm, bdv, 4)]

    with jax.named_scope("place"):
        ids = ids_ref[...].astype(F32)
        eye = lax.broadcasted_iota(jnp.int32, (tok, tok), 0) == lax.broadcasted_iota(jnp.int32, (tok, tok), 1)
        ids_c = jnp.sum(jnp.where(eye, jnp.broadcast_to(ids, (tok, tok)), 0.0), axis=1, keepdims=True)
        per_owner = stack // rank

        def fdiv(v, n):
            return jnp.floor((v + 0.5) * (1.0 / n))

        def place(v):
            owner = fdiv(v, per_owner)
            local = v - owner * per_owner
            oy = fdiv(owner, CORES * side)
            ox = fdiv(owner, CORES) - oy * side
            oc = owner - fdiv(owner, CORES) * CORES

            def mod(a, b, n):
                d = a - b.astype(F32)
                return jnp.where(d < 0, d + n, d)
            rel = (mod(oy, my_y, side) * side + mod(ox, my_x, side)) * CORES + mod(oc, my_c, CORES)
            return owner, local, rel

        own_r, _, rel_r = place(ids)
        own_c, loc_c, rel_c = place(ids_c)
        t0 = lax.broadcasted_iota(jnp.int32, (tok, tok), 0)
        t1 = lax.broadcasted_iota(jnp.int32, (tok, tok), 1)
        same = own_c == own_r
        arr_r = jnp.sum(jnp.where(same & (t0 < t1), 1.0, 0.0), axis=0, keepdims=True)
        arr_c = jnp.sum(jnp.where(same & (t1 < t0), 1.0, 0.0), axis=1, keepdims=True)

        def rows_of(rel, arr):
            main = (rel * slab + arr).astype(jnp.int32)
            tail_row = fdiv(arr, third)
            tail = (rel * slab + cap + tail_row).astype(jnp.int32)
            part = (arr - tail_row * third).astype(jnp.int32)
            return main, tail, part

        main_r, tail_r, part_r = rows_of(rel_r, arr_r)
        main_c, tail_c, part_c = rows_of(rel_c, arr_c)
        s_main = one_hot(packed, tok, lambda r, c: r == main_r)
        s_tail = [one_hot(packed, tok, lambda r, c: (r == tail_r) & (part_r == k)) for k in range(third)]
        gmat[0] = one_hot(tok, packed, lambda r, c: c == main_c)
        for k in range(third):
            gmat[1 + k] = one_hot(tok, packed, lambda r, c: (c == tail_c) & (part_c == k))
        mine = one_hot(tok, stack, lambda r, c: loc_c == fdiv(c.astype(F32), rank))

    with jax.named_scope("x_wait"):
        x_copy.wait()
    with jax.named_scope("weights"):
        for p in range(2):
            for u in range(UNITS // 2):
                fill(p, 0, u, p * (UNITS // 2) + u)

    n_pass = len(passes)

    def copy1(p, r):
        q, dc = r // CORES, r % CORES
        if p == n_pass:
            src, dst = sendm.at[q, dc], recvm.at[q, dc]
        else:
            at = pl.ds(*passes[p])
            src, dst = sendx.at[at, q, dc], recvx.at[at, q, dc]
        near = int(q == 0)
        return remote(src, dst, s1_sem.at[int(p == n_pass), near], r1_sem.at[p, near], target(r))

    others = pl.ds(1, chips - 1)

    def all_of(ref, ssem, rsem):
        return remote(ref, ref, ssem, rsem, target(1))

    for p in range(n_pass + 1):
        with jax.named_scope(f"pack{p}"):
            if p == n_pass:
                sendm[...] = dot(s_main, mine).reshape(chips, CORES, slab, stack).astype(BF)
            else:
                for b in range(passes[p][0], sum(passes[p])):
                    xa = x_v[:, b * UNIT_N:b * UNIT_N + MAIN]
                    xb = x_v[:, b * UNIT_N + MAIN:(b + 1) * UNIT_N]
                    both = dot(s_main, xa) + jnp.concatenate([dot(s, xb) for s in s_tail], axis=1)
                    sendx[b] = both.reshape(chips, CORES, slab, MAIN).astype(BF)
        if p == 0:
            with jax.named_scope("bar_wait"):
                pl.semaphore_wait(barrier, groups - 1)
        with jax.named_scope(f"send{p}"):
            for r in order:
                copy1(p, r).start()
            if p == n_pass:
                recvm[0, 0] = sendm[0, 0]
            else:
                for b in range(passes[p][0], sum(passes[p])):
                    recvx[b, 0, 0] = sendx[b, 0, 0]

    def slot_of(s):
        g = fdiv(s.astype(F32), cap).astype(jnp.int32)
        return g, s - g * cap

    def unpack_main(r, c):
        g, j = slot_of(r)
        return c == g * slab + j

    def unpack_tail(k):
        def hit(r, c):
            g, j = slot_of(r)
            q = fdiv(j.astype(F32), third).astype(jnp.int32)
            return (c == g * slab + cap + q) & (j - q * third == k)
        return hit

    def pack_main(r, c):
        return unpack_main(c, r)

    def pack_tail(k):
        def hit(r, c):
            return unpack_tail(k)(c, r)
        return hit

    with jax.named_scope("maps"):
        unmap[0] = one_hot(slots, packed, unpack_main)
        remap[0] = one_hot(packed, slots, pack_main)
        for k in range(third):
            unmap[1 + k] = one_hot(slots, packed, unpack_tail(k))
            remap[1 + k] = one_hot(packed, slots, pack_tail(k))
    w = MAIN // third

    def dense(v):
        return v.astype(F32).reshape(packed, v.shape[-1]).astype(BF)

    def arrive(p):
        with jax.named_scope(f"recv{p}"):
            if p == n_pass:
                all_of(recvm.at[others], s1_sem.at[1, 0], r1_sem.at[p, 0]).wait_recv()
                all_of(recvm.at[0, 1], s1_sem.at[1, 1], r1_sem.at[p, 1]).wait_recv()
            else:
                at = pl.ds(*passes[p])
                all_of(recvx.at[at, others], s1_sem.at[0, 0], r1_sem.at[p, 0]).wait_recv()
                all_of(recvx.at[at, 0, 1], s1_sem.at[0, 1], r1_sem.at[p, 1]).wait_recv()
        with jax.named_scope(f"unpack{p}"):
            if p == n_pass:
                keep_v[...] = dot(unmap[0], dense(recvm[...]))
            else:
                for b in range(passes[p][0], sum(passes[p])):
                    part = dense(recvx[b])
                    xc[:, b * UNIT_N:b * UNIT_N + MAIN] = dot(unmap[0], part).astype(BF)
                    tail = sum(dot(unmap[1 + k], part[:, k * w:(k + 1) * w]) for k in range(third))
                    xc[:, b * UNIT_N + MAIN:(b + 1) * UNIT_N] = tail.astype(BF)

    def pick(low):
        return jnp.where(keep_v[...] > 0.5, low.astype(BF).astype(F32), 0.0).astype(BF)

    for p in range(n_pass):
        arrive(p)
        c, n = passes[p]
        rows = n * UNIT_N
        if p == last_pass:
            arrive(n_pass)
            pl.semaphore_signal(free_sem, inc=1, device_id=device(0, 0, 1), device_id_type=pl.DeviceIdType.MESH)
            with jax.named_scope("low"):
                down = h_v.at[pl.ds(0, stack), pl.ds(0, 2 * dim)]
                in_copy(down, down, 1).wait()
                in_copy(bgu, bgu, 2).wait()
                for i in range(2):
                    low_v[i] = pick(sum(dot_t(xc[:, k:k + UNIT_N], h_v[0:stack, i * dim + k:i * dim + k + UNIT_N]) for k in range(0, dim, UNIT_N)))
        start = p * (UNITS // 2) if n == 1 else 0
        size = (GROUPS if n == 1 else 1) * per_step
        blocks = size if n == 1 else size // 2

        def step(i, carry):
            base = i * size
            if n == 1:
                for g in range(GROUPS):
                    filled(start + base + g * per_step)
            with jax.named_scope(f"dot{p}"):
                for b in range(blocks):
                    if n > 1 and b * size // blocks % per_step == 0:
                        filled(start + base + b * size // blocks)
                    for s in range(UNIT_N // 256):
                        col = pl.ds(pl.multiple_of((i * blocks + b) * UNIT_N + s * 256, 256), 256)
                        res = []
                        for which in range(2):
                            slot, row = (start + base + b, which * rows) if n == 1 else (base + b * 2 + which, 0)
                            d = dot(xc[:, c * UNIT_N:c * UNIT_N + rows], ring[slot, row:row + rows, s * 256:(s + 1) * 256])
                            if p > 0:
                                d = acc_v[which, :, col] + d
                            if p < last_pass:
                                acc_v[which, :, col] = d
                            else:
                                res.append(d + (scale * dot(low_v[which], bgu[which, :, col])).astype(BF).astype(F32))
                        if res:
                            g, u = res
                            h_v[:, col] = (g * (1.0 / (1.0 + jnp.exp(-g))) * u).astype(BF)
                    if (b + 1) * size // blocks % per_step:
                        continue
                    for k in range((b + 1) * size // blocks - per_step, (b + 1) * size // blocks):
                        slot = start + base + k
                        if p == last_pass:
                            out_unit(i * size // per_step + k // per_step, k % per_step, slot).start()
                        elif p == 0:
                            fill(2, base, k, slot)
                        elif p == 1:
                            fill(2, base + UNITS // 2, k, slot)
                        else:
                            fill(p + 1, base, k, slot)
            return carry

        steps = (UNITS // 2 if n == 1 else UNITS) // size
        if p == last_pass:
            for cp in late:
                cp.start()
        if steps == 1:
            step(0, 0)
        else:
            lax.fori_loop(0, steps, step, 0)
        if p == 1:
            for cp in early:
                cp.start()

    with jax.named_scope("low2"):
        for cp in late:
            cp.wait()
        @pl.when(me >= 0)
        def _():
            low_v[0] = pick(sum(dot_t(h_v[:, k:k + UNIT_K], adv[:, k:k + UNIT_K]) for k in range(0, ff, UNIT_K)))
    all_of(sendx.at[:, others], s1_sem.at[0, 0], r1_sem.at[0, 0]).wait_send()
    all_of(sendx.at[:, 0, 1], s1_sem.at[0, 1], r1_sem.at[0, 1]).wait_send()
    all_of(sendm.at[others], s1_sem.at[1, 0], r1_sem.at[0, 0]).wait_send()
    all_of(sendm.at[0, 1], s1_sem.at[1, 1], r1_sem.at[0, 1]).wait_send()

    def ship(n):
        with jax.named_scope(f"ship{n}"):
            for r in order:
                q, dc = r // CORES, r % CORES
                near = int(q == 0)
                remote(sendx.at[n, q, dc], land.at[n, q, dc], s2_sem.at[near], land_sem.at[n, near], target(r, True)).start()

    chip_order = [r // CORES for r in order if r % CORES == 0]

    def ship_pairs(n):
        with jax.named_scope(f"shipp{n}"):
            for q in chip_order:
                remote(sendx.at[n, q], land.at[n, q], s2_sem.at[2], land_sem.at[n, 0], target(q * CORES, True)).start()

    def hand_on(n):
        with jax.named_scope(f"hand{n}"):
            all_of(land.at[n, others], s2_sem.at[2], land_sem.at[n, 0]).wait_recv()
            if n == 0:
                pl.semaphore_wait(free_sem, 1)
            remote(land.at[n, :, 1], recvx.at[n, :, 1], s2_sem.at[3], part_sem.at[n], device(0, 0, 1)).start()

    def home(n):
        with jax.named_scope(f"homewait{n}"):
            if n < n_out - 1:
                all_of(recvx.at[n, :, 1], s2_sem.at[3], part_sem.at[n]).wait_recv()
                slabs = jnp.concatenate([land[n, :, 0:1], recvx[n, :, 1:2]], axis=1)
            else:
                all_of(land.at[n, others], s2_sem.at[0], land_sem.at[n, 0]).wait_recv()
                all_of(land.at[n, 0, 1], s2_sem.at[1], land_sem.at[n, 1]).wait_recv()
                slabs = land[n]
        with jax.named_scope(f"home{n}"):
            part = dense(slabs)
            x_v[:, n * UNIT_N:n * UNIT_N + MAIN] = dot(gmat[0], part).astype(BF)
            tail = sum(dot(gmat[1 + k], part[:, k * w:(k + 1) * w]) for k in range(third))
            x_v[:, n * UNIT_N + MAIN:(n + 1) * UNIT_N] = tail.astype(BF)
        cols = pl.ds(n * UNIT_N, UNIT_N)
        in_copy(x_v.at[:, cols], out_hbm.at[:, cols], 5).start()

    for n in range(n_out):
        base = n * k_out
        filled(base % UNITS)
        if n > 0:
            ship_pairs(n - 1)
        if n > 3:
            hand_on(n - 4)
        with jax.named_scope(f"out{n}"):
            done = []
            for s in range(UNIT_N // 256):
                cols = slice(n * UNIT_N + s * 256, n * UNIT_N + (s + 1) * 256)
                acc = None
                for k in range(k_out):
                    d = dot(h_v[:, k * UNIT_K:(k + 1) * UNIT_K], ring[(base + k) % UNITS, :, s * 256:(s + 1) * 256])
                    acc = d if acc is None else acc + d
                delta = (scale * dot(low_v[0], bdv[:, cols])).astype(BF).astype(F32)
                done.append((xc[:, cols].astype(F32) + (acc + delta)).astype(BF))
            done = jnp.concatenate(done, axis=1)
            both = dot(remap[0], done[:, :MAIN]) + jnp.concatenate([dot(remap[1 + k], done[:, MAIN:]) for k in range(third)], axis=1)
            sendx[n] = both.reshape(chips, CORES, slab, MAIN).astype(BF)
            if n < n_out - 1:
                land[n, 0] = sendx[n, 0]
            else:
                land[n, 0, 0] = sendx[n, 0, 0]
        ahead = n + UNITS // k_out
        for k in range(k_out):
            if ahead < n_out:
                out_unit(ahead, k, (base + k) % UNITS).start()
    m = n_out - 1
    ship(m)
    for n in range(m - 3, m):
        hand_on(n)
    for n in range(n_out):
        home(n)
    in_copy(x_v, out_hbm, 5).wait()
    all_of(sendx.at[m, others], s2_sem.at[0], land_sem.at[0, 0]).wait_send()
    all_of(sendx.at[m, 0, 1], s2_sem.at[1], land_sem.at[0, 1]).wait_send()
    all_of(sendx.at[pl.ds(0, m), others], s2_sem.at[2], land_sem.at[0, 0]).wait_send()
    all_of(land.at[pl.ds(0, m), :, 1], s2_sem.at[3], part_sem.at[0]).wait_send()


def solution(mesh):
    groups = mesh.shape["data"]
    row_spec = P(("rep", "data"), None)
    id_spec = P(("rep", "data"))
    owned_spec = P("data", None, None)

    def device_step(x, adapter_id, w_gate, w_up, w_down, a_gate, b_gate, a_up, b_up, a_down, b_down):
        tok, dim = x.shape
        ff = w_gate.shape[1]
        per_owner, rank, _ = a_gate.shape
        stack = per_owner * rank
        cap = (3 * tok + groups - 1) // groups
        slots = groups * cap
        slab = 8
        n_out = dim // UNIT_N
        chips = groups // CORES
        flat = [m.reshape(stack, m.shape[2]) for m in (a_gate, b_gate, a_up, b_up, a_down, b_down)]
        anyspec = pl.BlockSpec(memory_space=pl.ANY)
        dma = pltpu.SemaphoreType.DMA
        return pl.pallas_call(
            functools.partial(layer, groups, cap, LORA_ALPHA / rank, rank),
            out_shape=jax.ShapeDtypeStruct((tok, dim), BF),
            in_specs=[pl.BlockSpec(memory_space=pltpu.VMEM)] + [anyspec] * 10,
            out_specs=anyspec,
            scratch_shapes=[
                pltpu.VMEM((UNITS, UNIT_K, UNIT_N), BF),
                pltpu.VMEM((2, slots, ff), F32),
                pltpu.VMEM((tok, dim), BF),
                pltpu.VMEM((slots, dim), BF),
                pltpu.VMEM((slots, ff), BF),
                pltpu.VMEM((2, stack, ff), BF),
                pltpu.VMEM((stack, ff), BF),
                pltpu.VMEM((stack, dim), BF),
                pltpu.VMEM((n_out, chips, CORES, slab, MAIN), BF),
                pltpu.VMEM((n_out, chips, CORES, slab, MAIN), BF),
                pltpu.VMEM((chips, CORES, slab, stack), BF),
                pltpu.VMEM((chips, CORES, slab, stack), BF),
                pltpu.VMEM((n_out, chips, CORES, slab, MAIN), BF),
                pltpu.VMEM((slots, stack), F32),
                pltpu.VMEM((2, slots, stack), BF),
                pltpu.VMEM((1 + cap // 2, tok, groups * slab), BF),
                pltpu.VMEM((1 + cap // 2, slots, groups * slab), BF),
                pltpu.VMEM((1 + cap // 2, groups * slab, slots), BF),
                dma((UNITS // 8,)), dma((6,)), dma((2, 2)), dma((n_out - 1, 2)), dma((4,)), dma((n_out, 2)), dma((n_out - 1,)), pltpu.SemaphoreType.REGULAR,
            ],
            compiler_params=pltpu.CompilerParams(collective_id=0, has_side_effects=True, vmem_limit_bytes=67043328),
            name="lora_swiglu",
        )(adapter_id.reshape(1, tok), x, w_gate, w_up, w_down, *flat)

    return jax.shard_map(device_step, mesh=mesh, in_specs=(row_spec, id_spec, P(), P(), P(), owned_spec, owned_spec, owned_spec, owned_spec, owned_spec, owned_spec), out_specs=row_spec, check_vma=False)
```
